32 devices in a mesh: batch: 8 (over z, y), cols: 2 (over core), ens: 2 (over x).
Axes of the slice: x: 2, y: 2, z: 4, core: 2. Of those that a mesh axis runs over, the one named last changes fastest.
Arguments:
- slope_up: float32 [16, 1280, 5120], P(('ens', 'batch'), None, 'cols'), parts along dimension 0, may hold values from -0.875 to 0.875
- slope_down: float32 [16, 5120, 1280], P(('ens', 'batch'), 'cols'), parts along dimension 0, may hold values from -0.875 to 0.875
- slope_norm: float32 [16, 1280], P(('ens', 'batch')), parts along dimension 0, may hold values from -8 to 8
- slope_bias: float32 [16, 1280], P(('ens', 'batch')), parts along dimension 0, may hold values from -8 to 8
- param_up: float32 [2560, 5120], P(('ens', 'batch'), 'cols'), parts along dimension 0, may hold values from -0.25 to 0.25
- param_down: float32 [10240, 1280], P(('ens', 'cols'), 'batch'), parts along dimension 0, may hold values from -0.125 to 0.125
- param_norm: float32 [2560], P(('ens', 'batch')), parts along dimension 0, may hold values from 0.25 to 1.75
- param_bias: float32 [2560], P(('ens', 'batch')), parts along dimension 0, may hold values from -3 to 3
Outputs:
- half_up: bfloat16 [2560, 5120], P('ens', 'cols'), parts along dimension 0
- half_down: bfloat16 [10240, 1280], P(('ens', 'cols')), parts along dimension 0
- half_norm: bfloat16 [2560], P('ens'), parts along dimension 0
- half_bias: bfloat16 [2560], P('ens'), parts along dimension 0
- next_up: float32 [2560, 5120], P(('ens', 'batch'), 'cols'), parts along dimension 0
- next_down: float32 [10240, 1280], P(('ens', 'cols'), 'batch'), parts along dimension 0
- next_norm: float32 [2560], P(('ens', 'batch')), parts along dimension 0
- next_bias: float32 [2560], P(('ens', 'batch')), parts along dimension 0
The draws below stay inside these ranges and needn't reach their ends.
There are 2 independent parts, one for each index of `ens`. The reference program is written for one: setup_inputs(seed, part) draws one part's arguments, and reference() takes and returns one part's arrays. A program takes and returns all parts, laid end to end along the dimension named above; each array names one. Nothing has to cross between parts.
All inputs are finite; a program needn't handle non-finite values.
Results may differ from the reference program's by a relative error of at most 0.008.
Values may be sent and summed in bfloat16 or wider, within the bound.
A program may use at most 128 MiB of HBM per device.

```python
import jax
import jax.numpy as jnp
from jax import lax

WIDTH = 1280
INNER = 5120
REPLICAS = 8


def spiked(values, rng, source, target, shards_of, factor):
    owner, partner = [(jnp.arange(values.shape[position]) // (values.shape[position] // shards_of)).reshape([-1 if axis == position else 1 for axis in range(values.ndim)]) for position in (source, target)]
    chosen = jax.random.permutation(rng, shards_of)[partner]
    strong = (owner == chosen) | (owner == (partner + shards_of // 2) % shards_of)
    return jnp.where(strong, factor * values, values)


def block_levels(rng, dims, shards, low, high):
    loudness = 1.0
    for dim, blocks in shards:
        steps = jax.random.uniform(jax.random.fold_in(jax.random.fold_in(rng, 6), dim), (blocks,), jnp.float32, low / len(shards), high / len(shards))
        loudness = loudness * jnp.repeat(jnp.exp(steps), dims[dim] // blocks).reshape((-1,) + (1,) * (len(dims) - 1 - dim))
    return loudness


def bell_draw(key, dims, width, limit, shards=(), dtype=jnp.bfloat16):
    level = block_levels(key, dims, shards, -0.22, 0.18) if shards else 1.0
    drawn = jax.random.normal(key, dims, jnp.float32) * width * level
    return jnp.minimum(jnp.maximum(drawn, -limit), limit).astype(dtype)


def gaussian_with(key, extent, spread, most, shards, heavy, dtype=jnp.bfloat16):
    result = spread * jax.random.normal(key, extent, jnp.float32)
    if shards:
        result = result * block_levels(key, extent, shards, -0.22, 0.18)
    return jnp.clip(spiked(result, jax.random.fold_in(key, 3), *heavy), -most, most).astype(dtype)


def setup_inputs(seed: int = 0, part: int = 0) -> dict:
    streams_of = jax.random.split(jax.random.key(seed), 9)
    part_keys = jax.random.split(jax.random.fold_in(streams_of[8], part), 9)
    return {
        "slope_up": gaussian_with(part_keys[0], (REPLICAS, WIDTH, INNER), 0.1, 0.875, ((0, 8), (2, 2)), (0, 1, 8, 2.0), jnp.float32),
        "slope_down": gaussian_with(part_keys[1], (REPLICAS, INNER, WIDTH), 0.1, 0.875, ((0, 8), (1, 2)), (0, 2, 8, 2.0), jnp.float32),
        "slope_norm": gaussian_with(part_keys[2], (REPLICAS, WIDTH), 1.0, 8.0, ((0, 8),), (0, 1, 8, 2.0), jnp.float32),
        "slope_bias": gaussian_with(part_keys[3], (REPLICAS, WIDTH), 1.0, 8.0, ((0, 8),), (0, 1, 8, 2.0), jnp.float32),
        "param_up": gaussian_with(part_keys[4], (WIDTH, INNER), WIDTH ** -0.5, 0.25, ((0, 8), (1, 2)), (1, 0, 8, 2.0), jnp.float32),
        "param_down": gaussian_with(part_keys[5], (INNER, WIDTH), INNER ** -0.5, 0.125, ((0, 2), (1, 8)), (0, 1, 8, 2.0), jnp.float32),
        "param_norm": jnp.clip(1.0 + 0.15 * jax.random.normal(part_keys[6], (WIDTH,), jnp.float32), 0.25, 1.75),
        "param_bias": bell_draw(part_keys[7], (WIDTH,), 0.5, 3.0, ((0, 8),), jnp.float32),
    }


learn_rate = 0.4

def reference(slope_up, slope_down, slope_norm, slope_bias, param_up, param_down, param_norm, param_bias):
    mean_up = lax.optimization_barrier(jnp.sum(slope_up.astype(jnp.float32), axis=0)) * REPLICAS ** (-0.5)
    mean_down = lax.optimization_barrier(jnp.sum(slope_down.astype(jnp.float32), axis=0)) * REPLICAS ** (-0.5)
    mean_norm = lax.optimization_barrier(jnp.sum(slope_norm.astype(jnp.float32), axis=0)) * REPLICAS ** (-0.5)
    mean_bias = lax.optimization_barrier(jnp.sum(slope_bias.astype(jnp.float32), axis=0)) * REPLICAS ** (-0.5)
    ratio_up = jnp.sqrt(lax.optimization_barrier(jnp.sum(param_up * param_up, axis=1, keepdims=True))) * lax.rsqrt(lax.optimization_barrier(jnp.sum(mean_up * mean_up, axis=1, keepdims=True)) + 1e-06)
    mean_up = mean_up * ratio_up
    ratio_down = jnp.sqrt(lax.optimization_barrier(jnp.sum(param_down * param_down, axis=0, keepdims=True))) * lax.rsqrt(lax.optimization_barrier(jnp.sum(mean_down * mean_down, axis=0, keepdims=True)) + 1e-06)
    mean_down = mean_down * ratio_down
    next_up = param_up - learn_rate * mean_up
    next_down = param_down - learn_rate * mean_down
    next_norm = param_norm - learn_rate * mean_norm
    next_bias = param_bias - learn_rate * mean_bias
    half_up = next_up.astype(jnp.bfloat16)
    half_down = next_down.astype(jnp.bfloat16)
    half_norm = next_norm.astype(jnp.bfloat16)
    half_bias = next_bias.astype(jnp.bfloat16)
    return (half_up, half_down, half_norm, half_bias, next_up, next_down, next_norm, next_bias)
```

```python
import functools
import math

import jax
import jax.numpy as jnp
from jax import lax
from jax.experimental import pallas as pl
from jax.experimental.pallas import tpu as pltpu
from jax.sharding import PartitionSpec as P

learn_rate = 0.4
MESH = pl.DeviceIdType.MESH
R = 8
LANE = 128
SPLIT = 0.6
VMEM_BYTES = 66_000_000
F32, BF16 = jnp.float32, jnp.bfloat16


def kernel(
    n,
    m,
    LA,
    up_ref,
    down_ref,
    pup_ref,
    pdown_ref,
    vec_ref,
    G,
    T,
    NX,
    sums_ref,
    stage,
    turn,
    XA,
    XB,
    RYA,
    RYB,
    RZA,
    RZB,
    PR,
    SQ,
    VY,
    VZ,
    up_sem,
    down_sem,
    par_sem,
    send,
    recv,
    sq_send,
    sq_recv,
    v_send,
    v_recv,
):
    Z = n // 2
    C = NX.shape[0]
    CH = C // 2
    H0 = CH // 2
    L = NX.shape[2]
    me = lax.axis_index("batch")
    core = lax.axis_index("cols")
    z = me // 2
    y = me % 2
    other = z * 2 + 1 - y
    rate = n ** (-0.5)

    def slot(p):
        return jnp.where(p < H0, p, jnp.where(p < H0 + CH, p - H0 + CH, p - CH))

    def load_up(c):
        return pltpu.make_async_copy(up_ref.at[:, :, c], stage.at[c % 2], up_sem.at[c % 2])

    blocks = L // LANE
    share = -(-blocks // H0)
    back = -(-blocks // (CH - H0))

    def load_down(b):
        return pltpu.make_async_copy(
            down_ref.at[pl.ds(b * LANE, LANE)], turn.at[b % 2], down_sem.at[b % 2]
        )

    def turn_block(b):
        def pieces(store):
            for j in range(n * CH * R // LANE):
                tile = turn[b % 2, :, j * LANE : (j + 1) * LANE].T
                for i in range(LANE // R):
                    piece = j * (LANE // R) + i
                    d, k = piece // CH, piece % CH
                    store(d // 2, d % 2, CH + k, tile[i * R : (i + 1) * R].astype(BF16))

        @pl.when(b * LANE < LA)
        def _():
            at = pl.ds(pl.multiple_of(b * LANE, LANE), LANE)

            def store(d, v, c, x):
                XA[c, v, d, :, at] = x

            pieces(store)

        @pl.when(b * LANE >= LA)
        def _():
            at = pl.ds(pl.multiple_of(b * LANE - LA, LANE), LANE)

            def store(d, v, c, x):
                XB[c, d, v, :, at] = x

            pieces(store)

    def load_params():
        return [
            pltpu.make_async_copy(pup_ref, PR.at[pl.ds(0, CH)], par_sem.at[0]),
            pltpu.make_async_copy(pdown_ref, PR.at[pl.ds(CH, CH)], par_sem.at[1]),
        ]

    load_up(0).start()
    for d in load_params():
        d.start()

    load_down(0).start()

    barrier = pltpu.get_barrier_semaphore()
    for o in range(1, n):
        pl.semaphore_signal(
            barrier, inc=1, device_id={"batch": (me + o) % n}, device_id_type=MESH
        )
    for o in range(1, m):
        pl.semaphore_signal(
            barrier, inc=1, device_id={"cols": (core + o) % m}, device_id_type=MESH
        )
    pl.semaphore_wait(barrier, n - 1 + m - 1)

    def remote(src, dst, kind, c, to):
        return pltpu.make_async_remote_copy(
            src_ref=src,
            dst_ref=dst,
            send_sem=send.at[kind, c],
            recv_sem=recv.at[kind, c],
            device_id={"batch": to},
            device_id_type=MESH,
        )

    vec_y = pltpu.make_async_remote_copy(
        src_ref=vec_ref,
        dst_ref=VY,
        send_sem=v_send.at[0],
        recv_sem=v_recv.at[0],
        device_id={"batch": other},
        device_id_type=MESH,
    )
    vec_y.start()

    def vec_z(o):
        return pltpu.make_async_remote_copy(
            src_ref=VZ.at[z],
            dst_ref=VZ.at[z],
            send_sem=v_send.at[o],
            recv_sem=v_recv.at[o],
            device_id={"batch": (me + 2 * o) % n},
            device_id_type=MESH,
        )

    def sq_copy(c, o):
        return pltpu.make_async_remote_copy(
            src_ref=SQ.at[c, 0],
            dst_ref=SQ.at[c, o],
            send_sem=sq_send.at[o - 1, c],
            recv_sem=sq_recv.at[o - 1, c],
            device_id={"cols": (core + o) % m},
            device_id_type=MESH,
        )

    YA, YB, RA, LFA, RB, LFB, GYA, GYB, GRA, GLA, GRB, GLB = range(12)

    def ya(c):
        return remote(XA.at[c, 1 - y], RYA.at[c], YA, c, other)

    def yb(c):
        return remote(XB.at[c, z, 1 - y], RYB.at[c], YB, c, other)

    def gya(c):
        ref = G.at[:, y, c, :, pl.ds(0, LA)]
        return remote(ref, ref, GYA, c, other)

    def gya_in(c):
        ref = G.at[:, 1 - y, c, :, pl.ds(0, LA)]
        return remote(ref, ref, GYA, c, other)

    def gyb(c):
        ref = G.at[z, y, c, :, pl.ds(LA, L - LA)]
        return remote(ref, ref, GYB, c, other)

    def gyb_in(c):
        ref = G.at[z, 1 - y, c, :, pl.ds(LA, L - LA)]
        return remote(ref, ref, GYB, c, other)

    def x_ref(first, c):
        return XA.at[c, y] if first else XB.at[c]

    def sum_right(first, c, k):
        rz = RZA if first else RZB
        return remote(
            x_ref(first, c).at[pl.ds(k + 1, Z - 1 - k)],
            rz.at[c, pl.ds(k + 2, Z - 1 - k)],
            RA if first else RB,
            c,
            jnp.minimum(me + 2, n - 1),
        )

    def sum_left(first, c, k):
        rz = RZA if first else RZB
        return remote(
            x_ref(first, c).at[pl.ds(0, k)],
            rz.at[c, pl.ds(0, k)],
            LFA if first else LFB,
            c,
            jnp.maximum(me - 2, 0),
        )

    def add(first, c, lo, count, slot):
        rz = RZA if first else RZB
        for d in range(count):
            if first:
                XA[c, y, lo + d] = (
                    XA[c, y, lo + d].astype(F32) + rz[c, slot + d].astype(F32)
                ).astype(BF16)
            else:
                XB[c, lo + d] = (
                    XB[c, lo + d].astype(F32) + rz[c, slot + d].astype(F32)
                ).astype(BF16)

    def reduce_step(first, t):
        for k in range(Z):

            @pl.when((z == k) & (t - k >= 0) & (t - k < C))
            def _():
                c = slot(t - k)
                if k > 0:
                    sum_right(first, c, k - 1).wait_recv()
                    add(first, c, k, Z - k, k + 1)
                if k < Z - 1:
                    sum_right(first, c, k).start()

            q = Z - 1 - k

            @pl.when((z == k) & (t - q >= 0) & (t - q < C))
            def _():
                c = slot(t - q)
                if k < Z - 1:
                    sum_left(first, c, k + 1).wait_recv()
                    add(first, c, 0, k + 1, 0)
                if k > 0:
                    sum_left(first, c, k).start()

    def g_ref(first, c, lo, count):
        at = pl.ds(lo, count)
        if first:
            return G.at[at, y, c, :, pl.ds(0, LA)]
        return G.at[at, :, c, :, pl.ds(LA, L - LA)]

    def gather_right(first, c, k):
        ref = g_ref(first, c, 0, k + 1)
        return remote(ref, ref, GRA if first else GRB, c, jnp.minimum(me + 2, n - 1))

    def gather_left(first, c, k):
        ref = g_ref(first, c, k, Z - k)
        return remote(ref, ref, GLA if first else GLB, c, jnp.maximum(me - 2, 0))

    def gather_step(first, t):
        for k in range(Z):

            @pl.when((z == k) & (t - k >= 0) & (t - k < C))
            def _():
                c = slot(t - k)
                if k > 0:
                    gather_right(first, c, k - 1).wait_recv()
                if k < Z - 1:
                    gather_right(first, c, k).start()

            q = Z - 1 - k

            @pl.when((z == k) & (t - q >= 0) & (t - q < C))
            def _():
                c = slot(t - q)
                if k < Z - 1:
                    gather_left(first, c, k + 1).wait_recv()
                if k > 0:
                    gather_left(first, c, k).start()

    def back_block(b):
        at = pl.ds(pl.multiple_of(b * LANE, LANE), LANE)
        for j in range(n * CH * R // LANE):
            rows = []
            for i in range(LANE // R):
                piece = j * (LANE // R) + i
                d, k = piece // CH, piece % CH
                rows.append(G[d // 2, d % 2, CH + k, :, at].astype(F32))
            tile = jnp.concatenate(rows, axis=0)
            T[at, j * LANE : (j + 1) * LANE] = tile.T.astype(BF16)

    def lanes(x):
        s = x[:, :LANE] * x[:, :LANE]
        for i in range(1, L // LANE):
            part = x[:, i * LANE : (i + 1) * LANE]
            s = s + part * part
        return s

    def when_chunk(c):
        return pl.when((c >= 0) & (c < C))

    @pl.loop(0, C + 2 * Z)
    def _(t):
        def load_at(p, act):
            @pl.when((p < H0) | ((p >= H0 + CH) & (p < C)))
            def _():
                act(slot(p))

        load_at(t + 1, lambda c: load_up(c).start())

        def cast(c):
            load_up(c).wait()
            for d in range(Z):
                for v in range(2):
                    XA[c, v, d] = stage[c % 2, d, v, :, :LA].astype(BF16)
                    XB[c, d, v] = stage[c % 2, d, v, :, LA:].astype(BF16)

        load_at(t, cast)

        @pl.when(t < C)
        def _():
            ya(slot(t)).start()

        reduce_step(False, t)
        s = t - 1

        @pl.when(t == 1)
        def _():
            vec_y.wait()
            VZ[z] = vec_ref[...] + VY[...]
            for o in range(1, Z):
                vec_z(o).start()

        @when_chunk(s)
        def _():
            c = slot(s)
            ya(c).wait_recv()
            for d in range(Z):
                XA[c, y, d] = (XA[c, y, d].astype(F32) + RYA[c, d].astype(F32)).astype(BF16)

        reduce_step(True, s)
        b = t - (Z - 1)

        @when_chunk(b)
        def _():
            yb(slot(b)).start()

        u = t - Z

        @pl.when(u == 0)
        def _():
            for d in load_params():
                d.wait()

        @when_chunk(u)
        def _():
            f = slot(u)
            yb(f).wait_recv()
            NX[f, :, :LA] = XA[f, y, z].astype(F32) * rate
            NX[f, :, LA:] = (XB[f, z, y].astype(F32) + RYB[f].astype(F32)) * rate
            SQ[f, 0, 0] = lanes(NX[f])
            SQ[f, 0, 1] = lanes(PR[f])
            for o in range(1, m):
                sq_copy(f, o).start()

        @when_chunk(u - 1)
        def _():
            gyb_in(slot(u - 1)).wait_recv()

        gather_step(False, u - 1)
        e = u - Z

        @when_chunk(e)
        def _():
            gya_in(slot(e)).wait_recv()

        @when_chunk(u)
        def _():
            f = slot(u)
            for o in range(1, m):
                sq_copy(f, o).wait_recv()
            g = SQ[f, 0, 0]
            p = SQ[f, 0, 1]
            for o in range(1, m):
                g = g + SQ[f, o, 0]
                p = p + SQ[f, o, 1]
            g = jnp.sum(g, axis=1, keepdims=True)
            p = jnp.sum(p, axis=1, keepdims=True)
            scale = learn_rate * (jnp.sqrt(p) * lax.rsqrt(g + 1e-06))
            new = PR[f] - NX[f] * scale
            NX[f] = new
            G[z, y, f] = new.astype(BF16)
            gyb(f).start()

        gather_step(True, u)

        @when_chunk(u - (Z - 1))
        def _():
            gya(slot(u - (Z - 1))).start()

        for i in range(share):
            b = t * share + i

            @pl.when(b + 1 < blocks)
            def _():
                load_down(b + 1).start()

            @pl.when(b < blocks)
            def _():
                load_down(b).wait()
                turn_block(b)

        for i in range(back):
            w = (t - (H0 + CH + 2 * Z)) * back + i

            @pl.when((w >= 0) & (w < blocks))
            def _():
                back_block(w)

    for o in range(1, Z):
        vec_z(o).wait()
    total = VZ[0]
    for k in range(1, Z):
        total = total + VZ[k]
    sums_ref[...] = total

    @pl.loop(0, C)
    def _(c):
        for d in (ya(c), yb(c), gya(c), gyb(c)):
            d.wait_send()
        for o in range(1, m):
            sq_copy(c, o).wait_send()
        for k in range(Z):

            @pl.when(z == k)
            def _():
                for first in (True, False):
                    if k < Z - 1:
                        sum_right(first, c, k).wait_send()
                        gather_right(first, c, k).wait_send()
                    if k > 0:
                        sum_left(first, c, k).wait_send()
                        gather_left(first, c, k).wait_send()


def put_kernel(G, T, NX, half_up_ref, half_down_ref, next_up_ref, next_down_ref, sem):
    Z = G.shape[0]
    CH = G.shape[2] // 2
    part = T.shape[0] // (2 * Z)
    copies = []

    def put(src, dst):
        d = pltpu.make_async_copy(src, dst, sem.at[len(copies)])
        d.start()
        copies.append(d)

    for k in range(Z):
        for v in range(2):
            put(G.at[k, v, pl.ds(0, CH)], half_up_ref.at[k, v])
            at = pl.ds((2 * k + v) * part, part)
            put(T.at[at], half_down_ref.at[at])
    put(NX.at[pl.ds(0, CH)], next_up_ref)
    put(NX.at[pl.ds(CH, CH)], next_down_ref)
    for d in copies:
        d.wait()


def on_device(
    slope_up, slope_down, slope_norm, slope_bias, param_up, param_down, param_norm, param_bias
):
    n = lax.axis_size("batch")
    m = lax.axis_size("cols")
    Z = n // 2
    rows, L = param_up.shape
    CH = rows // R
    C = 2 * CH
    LA = max(1, round(SPLIT * L / LANE)) * LANE
    LB = L - LA
    width = slope_norm.shape[1]
    place = lax.axis_index("batch")
    up = slope_up[0].reshape(Z, 2, CH, R, L)
    down = slope_down[0]
    pup = param_up.reshape(CH, R, L)
    pdown = param_down.T.reshape(CH, R, L)
    mine = lax.dynamic_update_slice(
        jnp.zeros((2, width), F32), jnp.stack([param_norm, param_bias]), (0, place * rows)
    )
    vec = jnp.concatenate([slope_norm, slope_bias, mine], axis=0).reshape(8, width // 2)
    kinds = 12
    hbm = pl.BlockSpec(memory_space=pl.ANY)
    vmem = pl.BlockSpec(memory_space=pltpu.VMEM)
    kept = [((Z, 2, C, R, L), BF16), ((L, n * rows), BF16), ((C, R, L), F32)]
    size = sum(jnp.dtype(dtype).itemsize * math.prod(shape) for shape, dtype in kept)
    G, T, NX, sums = pl.pallas_call(
        functools.partial(kernel, n, m, LA),
        out_shape=tuple(pltpu.VMEM(shape, dtype) for shape, dtype in kept)
        + (jax.ShapeDtypeStruct(vec.shape, F32),),
        in_specs=[hbm, hbm, hbm, hbm, vmem],
        out_specs=(vmem, vmem, vmem, vmem),
        scratch_shapes=[
            pltpu.VMEM((2, Z, 2, R, L), F32),
            pltpu.VMEM((2, LANE, n * rows), F32),
            pltpu.VMEM((C, 2, Z, R, LA), BF16),
            pltpu.VMEM((C, Z, 2, R, LB), BF16),
            pltpu.VMEM((C, Z, R, LA), BF16),
            pltpu.VMEM((C, R, LB), BF16),
            pltpu.VMEM((C, Z + 1, R, LA), BF16),
            pltpu.VMEM((C, Z + 1, 2, R, LB), BF16),
            pltpu.VMEM((C, R, L), F32),
            pltpu.VMEM((C, m, 2, R, LANE), F32),
            pltpu.VMEM(vec.shape, F32),
            pltpu.VMEM((Z,) + vec.shape, F32),
            pltpu.SemaphoreType.DMA((2,)),
            pltpu.SemaphoreType.DMA((2,)),
            pltpu.SemaphoreType.DMA((2,)),
            pltpu.SemaphoreType.DMA((kinds, C)),
            pltpu.SemaphoreType.DMA((kinds, C)),
            pltpu.SemaphoreType.DMA((m - 1, C)),
            pltpu.SemaphoreType.DMA((m - 1, C)),
            pltpu.SemaphoreType.DMA((Z,)),
            pltpu.SemaphoreType.DMA((Z,)),
        ],
        compiler_params=pltpu.CompilerParams(
            collective_id=0, has_side_effects=True, vmem_limit_bytes=VMEM_BYTES - size
        ),
    )(up, down, pup, pdown, vec)
    half_up, half_down, new_up, new_down = pl.pallas_call(
        put_kernel,
        out_shape=(
            jax.ShapeDtypeStruct((Z, 2, CH, R, L), BF16),
            jax.ShapeDtypeStruct((L, n * rows), BF16),
            jax.ShapeDtypeStruct((CH, R, L), F32),
            jax.ShapeDtypeStruct((CH, R, L), F32),
        ),
        in_specs=[vmem] * 3,
        out_specs=(hbm,) * 4,
        scratch_shapes=[pltpu.SemaphoreType.DMA((4 * Z + 2,))],
        compiler_params=pltpu.CompilerParams(vmem_limit_bytes=1 << 20),
    )(*(pltpu.with_memory_space_constraint(x, pltpu.VMEM) for x in (G, T, NX)))
    half_up = half_up.reshape(n * rows, L)
    next_up = new_up.reshape(rows, L)
    next_down = new_down.reshape(rows, L).T
    sums = sums.reshape(4, width)
    whole = sums[2:] - learn_rate * (sums[:2] * n ** (-0.5))
    own = lax.dynamic_slice_in_dim(whole, place * rows, rows, axis=1)
    halves = whole.astype(BF16)
    return (half_up, half_down, halves[0], halves[1], next_up, next_down, own[0], own[1])


def solution(mesh):
    return jax.shard_map(
        on_device,
        mesh=mesh,
        in_specs=(
            P(("ens", "batch"), None, "cols"),
            P(("ens", "batch"), "cols", None),
            P(("ens", "batch"), None),
            P(("ens", "batch"), None),
            P(("ens", "batch"), "cols"),
            P(("ens", "cols"), "batch"),
            P(("ens", "batch")),
            P(("ens", "batch")),
        ),
        out_specs=(
            P("ens", "cols"),
            P(("ens", "cols"), None),
            P("ens"),
            P("ens"),
            P(("ens", "batch"), "cols"),
            P(("ens", "cols"), "batch"),
            P(("ens", "batch")),
            P(("ens", "batch")),
        ),
        check_vma=False,
    )
```

```python
import functools
import math

import jax
import jax.numpy as jnp
from jax import lax
from jax.experimental import pallas as pl
from jax.experimental.pallas import tpu as pltpu
from jax.sharding import PartitionSpec as P

learn_rate = 0.4
MESH = pl.DeviceIdType.MESH
R = 8
LANE = 128
SPLIT = 0.6
VMEM_BYTES = 66_000_000
F32, BF16 = jnp.float32, jnp.bfloat16


def kernel(
    n,
    m,
    LA,
    up_ref,
    down_ref,
    pup_ref,
    pdown_ref,
    norm_ref,
    bias_ref,
    pnorm_ref,
    pbias_ref,
    G,
    T,
    NX,
    sums_ref,
    stage,
    turn,
    XA,
    XB,
    RYA,
    RYB,
    RZA,
    RZB,
    PR,
    SQ,
    V,
    VP,
    VY,
    VZ,
    up_sem,
    down_sem,
    par_sem,
    send,
    recv,
    sq_send,
    sq_recv,
    v_send,
    v_recv,
):
    Z = n // 2
    C = NX.shape[0]
    CH = C // 2
    H0 = CH // 2
    L = NX.shape[2]
    me = lax.axis_index("batch")
    core = lax.axis_index("cols")
    z = me // 2
    y = me % 2
    other = z * 2 + 1 - y
    rate = n ** (-0.5)

    def slot(p):
        return jnp.where(p < H0, p, jnp.where(p < H0 + CH, p - H0 + CH, p - CH))

    def load_up(c):
        return pltpu.make_async_copy(up_ref.at[:, :, c], stage.at[c % 2], up_sem.at[c % 2])

    blocks = L // LANE
    share = -(-blocks // H0)
    back = -(-blocks // (CH - H0))

    def load_down(b):
        return pltpu.make_async_copy(
            down_ref.at[pl.ds(b * LANE, LANE)], turn.at[b % 2], down_sem.at[b % 2]
        )

    def turn_block(b):
        def pieces(store):
            for j in range(n * CH * R // LANE):
                tile = turn[b % 2, :, j * LANE : (j + 1) * LANE].T
                for i in range(LANE // R):
                    piece = j * (LANE // R) + i
                    d, k = piece // CH, piece % CH
                    store(d // 2, d % 2, CH + k, tile[i * R : (i + 1) * R].astype(BF16))

        @pl.when(b * LANE < LA)
        def _():
            at = pl.ds(pl.multiple_of(b * LANE, LANE), LANE)

            def store(d, v, c, x):
                XA[c, v, d, :, at] = x

            pieces(store)

        @pl.when(b * LANE >= LA)
        def _():
            at = pl.ds(pl.multiple_of(b * LANE - LA, LANE), LANE)

            def store(d, v, c, x):
                XB[c, d, v, :, at] = x

            pieces(store)

    def load_params():
        return [
            pltpu.make_async_copy(pup_ref, PR.at[pl.ds(0, CH)], par_sem.at[0]),
            pltpu.make_async_copy(pdown_ref, PR.at[pl.ds(CH, CH)], par_sem.at[1]),
        ]

    def load_vectors():
        return [
            pltpu.make_async_copy(norm_ref, V.at[0], par_sem.at[2]),
            pltpu.make_async_copy(bias_ref, V.at[1], par_sem.at[3]),
            pltpu.make_async_copy(pnorm_ref, VP.at[0], par_sem.at[4]),
            pltpu.make_async_copy(pbias_ref, VP.at[1], par_sem.at[5]),
        ]

    load_up(0).start()
    for d in load_params() + load_vectors():
        d.start()

    load_down(0).start()

    barrier = pltpu.get_barrier_semaphore()
    for o in range(1, n):
        pl.semaphore_signal(
            barrier, inc=1, device_id={"batch": (me + o) % n}, device_id_type=MESH
        )
    for o in range(1, m):
        pl.semaphore_signal(
            barrier, inc=1, device_id={"cols": (core + o) % m}, device_id_type=MESH
        )
    pl.semaphore_wait(barrier, n - 1 + m - 1)

    def remote(src, dst, kind, c, to):
        return pltpu.make_async_remote_copy(
            src_ref=src,
            dst_ref=dst,
            send_sem=send.at[kind, c],
            recv_sem=recv.at[kind, c],
            device_id={"batch": to},
            device_id_type=MESH,
        )

    def vec_y():
        return pltpu.make_async_remote_copy(
            src_ref=VZ.at[z],
            dst_ref=VY,
            send_sem=v_send.at[0],
            recv_sem=v_recv.at[0],
            device_id={"batch": other},
            device_id_type=MESH,
        )

    def vec_z(o):
        return pltpu.make_async_remote_copy(
            src_ref=VZ.at[z],
            dst_ref=VZ.at[z],
            send_sem=v_send.at[o],
            recv_sem=v_recv.at[o],
            device_id={"batch": (me + 2 * o) % n},
            device_id_type=MESH,
        )

    def sq_copy(c, o):
        return pltpu.make_async_remote_copy(
            src_ref=SQ.at[c, 0],
            dst_ref=SQ.at[c, o],
            send_sem=sq_send.at[o - 1, c],
            recv_sem=sq_recv.at[o - 1, c],
            device_id={"cols": (core + o) % m},
            device_id_type=MESH,
        )

    YA, YB, RA, LFA, RB, LFB, GYA, GYB, GRA, GLA, GRB, GLB = range(12)

    def ya(c):
        return remote(XA.at[c, 1 - y], RYA.at[c], YA, c, other)

    def yb(c):
        return remote(XB.at[c, z, 1 - y], RYB.at[c], YB, c, other)

    def gya(c):
        ref = G.at[:, y, c, :, pl.ds(0, LA)]
        return remote(ref, ref, GYA, c, other)

    def gya_in(c):
        ref = G.at[:, 1 - y, c, :, pl.ds(0, LA)]
        return remote(ref, ref, GYA, c, other)

    def gyb(c):
        ref = G.at[z, y, c, :, pl.ds(LA, L - LA)]
        return remote(ref, ref, GYB, c, other)

    def gyb_in(c):
        ref = G.at[z, 1 - y, c, :, pl.ds(LA, L - LA)]
        return remote(ref, ref, GYB, c, other)

    def x_ref(first, c):
        return XA.at[c, y] if first else XB.at[c]

    def sum_right(first, c, k):
        rz = RZA if first else RZB
        return remote(
            x_ref(first, c).at[pl.ds(k + 1, Z - 1 - k)],
            rz.at[c, pl.ds(k + 2, Z - 1 - k)],
            RA if first else RB,
            c,
            jnp.minimum(me + 2, n - 1),
        )

    def sum_left(first, c, k):
        rz = RZA if first else RZB
        return remote(
            x_ref(first, c).at[pl.ds(0, k)],
            rz.at[c, pl.ds(0, k)],
            LFA if first else LFB,
            c,
            jnp.maximum(me - 2, 0),
        )

    def add(first, c, lo, count, slot):
        rz = RZA if first else RZB
        for d in range(count):
            if first:
                XA[c, y, lo + d] = (
                    XA[c, y, lo + d].astype(F32) + rz[c, slot + d].astype(F32)
                ).astype(BF16)
            else:
                XB[c, lo + d] = (
                    XB[c, lo + d].astype(F32) + rz[c, slot + d].astype(F32)
                ).astype(BF16)

    def reduce_step(first, t):
        for k in range(Z):

            @pl.when((z == k) & (t - k >= 0) & (t - k < C))
            def _():
                c = slot(t - k)
                if k > 0:
                    sum_right(first, c, k - 1).wait_recv()
                    add(first, c, k, Z - k, k + 1)
                if k < Z - 1:
                    sum_right(first, c, k).start()

            q = Z - 1 - k

            @pl.when((z == k) & (t - q >= 0) & (t - q < C))
            def _():
                c = slot(t - q)
                if k < Z - 1:
                    sum_left(first, c, k + 1).wait_recv()
                    add(first, c, 0, k + 1, 0)
                if k > 0:
                    sum_left(first, c, k).start()

    def g_ref(first, c, lo, count):
        at = pl.ds(lo, count)
        if first:
            return G.at[at, y, c, :, pl.ds(0, LA)]
        return G.at[at, :, c, :, pl.ds(LA, L - LA)]

    def gather_right(first, c, k):
        ref = g_ref(first, c, 0, k + 1)
        return remote(ref, ref, GRA if first else GRB, c, jnp.minimum(me + 2, n - 1))

    def gather_left(first, c, k):
        ref = g_ref(first, c, k, Z - k)
        return remote(ref, ref, GLA if first else GLB, c, jnp.maximum(me - 2, 0))

    def gather_step(first, t):
        for k in range(Z):

            @pl.when((z == k) & (t - k >= 0) & (t - k < C))
            def _():
                c = slot(t - k)
                if k > 0:
                    gather_right(first, c, k - 1).wait_recv()
                if k < Z - 1:
                    gather_right(first, c, k).start()

            q = Z - 1 - k

            @pl.when((z == k) & (t - q >= 0) & (t - q < C))
            def _():
                c = slot(t - q)
                if k < Z - 1:
                    gather_left(first, c, k + 1).wait_recv()
                if k > 0:
                    gather_left(first, c, k).start()

    def back_block(b):
        at = pl.ds(pl.multiple_of(b * LANE, LANE), LANE)
        for j in range(n * CH * R // LANE):
            rows = []
            for i in range(LANE // R):
                piece = j * (LANE // R) + i
                d, k = piece // CH, piece % CH
                rows.append(G[d // 2, d % 2, CH + k, :, at].astype(F32))
            tile = jnp.concatenate(rows, axis=0)
            T[at, j * LANE : (j + 1) * LANE] = tile.T.astype(BF16)

    def lanes(x):
        s = x[:, :LANE] * x[:, :LANE]
        for i in range(1, L // LANE):
            part = x[:, i * LANE : (i + 1) * LANE]
            s = s + part * part
        return s

    def when_chunk(c):
        return pl.when((c >= 0) & (c < C))

    @pl.loop(0, C + 2 * Z)
    def _(t):
        def load_at(p, act):
            @pl.when((p < H0) | ((p >= H0 + CH) & (p < C)))
            def _():
                act(slot(p))

        load_at(t + 1, lambda c: load_up(c).start())

        def cast(c):
            load_up(c).wait()
            for d in range(Z):
                for v in range(2):
                    XA[c, v, d] = stage[c % 2, d, v, :, :LA].astype(BF16)
                    XB[c, d, v] = stage[c % 2, d, v, :, LA:].astype(BF16)

        load_at(t, cast)

        @pl.when(t < C)
        def _():
            ya(slot(t)).start()

        reduce_step(False, t)
        s = t - 1

        @pl.when(t == 0)
        def _():
            for d in load_vectors():
                d.wait()
            width = VY.shape[1]
            place = jnp.zeros((1, width - VP.shape[2]), F32)
            for i in range(2):
                VZ[z, i : i + 1] = V[i]
                own = jnp.concatenate([VP[i], place], axis=1)
                VZ[z, 2 + i : 3 + i] = pltpu.roll(own, me * VP.shape[2], 1)
            vec_y().start()

        @pl.when(t == 1)
        def _():
            vec_y().wait()
            VZ[z] = VZ[z] + VY[...]
            for o in range(1, Z):
                vec_z(o).start()

        @when_chunk(s)
        def _():
            c = slot(s)
            ya(c).wait_recv()
            for d in range(Z):
                XA[c, y, d] = (XA[c, y, d].astype(F32) + RYA[c, d].astype(F32)).astype(BF16)

        reduce_step(True, s)
        b = t - (Z - 1)

        @when_chunk(b)
        def _():
            yb(slot(b)).start()

        u = t - Z

        @pl.when(u == 0)
        def _():
            for d in load_params():
                d.wait()

        @when_chunk(u)
        def _():
            f = slot(u)
            yb(f).wait_recv()
            NX[f, :, :LA] = XA[f, y, z].astype(F32) * rate
            NX[f, :, LA:] = (XB[f, z, y].astype(F32) + RYB[f].astype(F32)) * rate
            SQ[f, 0, 0] = lanes(NX[f])
            SQ[f, 0, 1] = lanes(PR[f])
            for o in range(1, m):
                sq_copy(f, o).start()

        @when_chunk(u - 1)
        def _():
            gyb_in(slot(u - 1)).wait_recv()

        gather_step(False, u - 1)
        e = u - Z

        @when_chunk(u)
        def _():
            f = slot(u)
            for o in range(1, m):
                sq_copy(f, o).wait_recv()
            g = SQ[f, 0, 0]
            p = SQ[f, 0, 1]
            for o in range(1, m):
                g = g + SQ[f, o, 0]
                p = p + SQ[f, o, 1]
            g = jnp.sum(g, axis=1, keepdims=True)
            p = jnp.sum(p, axis=1, keepdims=True)
            scale = learn_rate * (jnp.sqrt(p) * lax.rsqrt(g + 1e-06))
            new = PR[f] - NX[f] * scale
            NX[f] = new
            G[z, y, f] = new.astype(BF16)
            gyb(f).start()

        gather_step(True, u)

        @when_chunk(u - (Z - 1))
        def _():
            gya(slot(u - (Z - 1))).start()

        @when_chunk(e)
        def _():
            gya_in(slot(e)).wait_recv()

        for i in range(share):
            b = t * share + i

            @pl.when(b + 1 < blocks)
            def _():
                load_down(b + 1).start()

            @pl.when(b < blocks)
            def _():
                load_down(b).wait()
                turn_block(b)

        for i in range(back):
            w = (t - (H0 + CH + 2 * Z)) * back + i

            @pl.when((w >= 0) & (w < blocks))
            def _():
                back_block(w)

    for o in range(1, Z):
        vec_z(o).wait()
    total = VZ[0]
    for k in range(1, Z):
        total = total + VZ[k]
    sums_ref[...] = total

    @pl.loop(0, C)
    def _(c):
        for d in (ya(c), yb(c), gya(c), gyb(c)):
            d.wait_send()
        for o in range(1, m):
            sq_copy(c, o).wait_send()
        for k in range(Z):

            @pl.when(z == k)
            def _():
                for first in (True, False):
                    if k < Z - 1:
                        sum_right(first, c, k).wait_send()
                        gather_right(first, c, k).wait_send()
                    if k > 0:
                        sum_left(first, c, k).wait_send()
                        gather_left(first, c, k).wait_send()


def put_kernel(
    G,
    T,
    NX,
    sums,
    half_up_ref,
    half_down_ref,
    half_norm_ref,
    half_bias_ref,
    next_up_ref,
    next_down_ref,
    next_norm_ref,
    next_bias_ref,
    sem,
):
    n = lax.axis_size("batch")
    me = lax.axis_index("batch")
    width = sums.shape[1]
    rows = width // n
    Z = G.shape[0]
    CH = G.shape[2] // 2
    part = T.shape[0] // (2 * Z)
    copies = []

    def put(src, dst):
        d = pltpu.make_async_copy(src, dst, sem.at[len(copies)])
        d.start()
        copies.append(d)

    for k in range(Z):
        for v in range(2):
            put(G.at[k, v, pl.ds(0, CH)], half_up_ref.at[k, v])
            at = pl.ds((2 * k + v) * part, part)
            put(T.at[at], half_down_ref.at[at])
    put(NX.at[pl.ds(0, CH)], next_up_ref)
    put(NX.at[pl.ds(CH, CH)], next_down_ref)
    whole = sums[2:4] - learn_rate * (sums[0:2] * n ** (-0.5))
    halves = whole.astype(BF16)
    half_norm_ref[...] = halves[0:1].reshape(width)
    half_bias_ref[...] = halves[1:2].reshape(width)
    own = pltpu.roll(whole, (n - me) % n * rows, 1)[:, :rows]
    next_norm_ref[...] = own[0:1].reshape(rows)
    next_bias_ref[...] = own[1:2].reshape(rows)
    for d in copies:
        d.wait()


def on_device(
    slope_up, slope_down, slope_norm, slope_bias, param_up, param_down, param_norm, param_bias
):
    n = lax.axis_size("batch")
    m = lax.axis_size("cols")
    Z = n // 2
    rows, L = param_up.shape
    CH = rows // R
    C = 2 * CH
    LA = max(1, round(SPLIT * L / LANE)) * LANE
    LB = L - LA
    width = slope_norm.shape[1]
    up = slope_up[0].reshape(Z, 2, CH, R, L)
    down = slope_down[0]
    pup = param_up.reshape(CH, R, L)
    pdown = param_down.T.reshape(CH, R, L)
    pnorm = param_norm.reshape(1, rows)
    pbias = param_bias.reshape(1, rows)
    kinds = 12
    hbm = pl.BlockSpec(memory_space=pl.ANY)
    vmem = pl.BlockSpec(memory_space=pltpu.VMEM)
    kept = [((Z, 2, C, R, L), BF16), ((L, n * rows), BF16), ((C, R, L), F32), ((4, width), F32)]
    size = sum(jnp.dtype(dtype).itemsize * math.prod(shape) for shape, dtype in kept)
    G, T, NX, sums = pl.pallas_call(
        functools.partial(kernel, n, m, LA),
        out_shape=tuple(pltpu.VMEM(shape, dtype) for shape, dtype in kept),
        in_specs=[hbm] * 8,
        out_specs=(vmem,) * 4,
        scratch_shapes=[
            pltpu.VMEM((2, Z, 2, R, L), F32),
            pltpu.VMEM((2, LANE, n * rows), F32),
            pltpu.VMEM((C, 2, Z, R, LA), BF16),
            pltpu.VMEM((C, Z, 2, R, LB), BF16),
            pltpu.VMEM((C, Z, R, LA), BF16),
            pltpu.VMEM((C, R, LB), BF16),
            pltpu.VMEM((C, Z + 1, R, LA), BF16),
            pltpu.VMEM((C, Z + 1, 2, R, LB), BF16),
            pltpu.VMEM((C, R, L), F32),
            pltpu.VMEM((C, m, 2, R, LANE), F32),
            pltpu.VMEM((2, 1, width), F32),
            pltpu.VMEM((2, 1, rows), F32),
            pltpu.VMEM((4, width), F32),
            pltpu.VMEM((Z, 4, width), F32),
            pltpu.SemaphoreType.DMA((2,)),
            pltpu.SemaphoreType.DMA((2,)),
            pltpu.SemaphoreType.DMA((6,)),
            pltpu.SemaphoreType.DMA((kinds, C)),
            pltpu.SemaphoreType.DMA((kinds, C)),
            pltpu.SemaphoreType.DMA((m - 1, C)),
            pltpu.SemaphoreType.DMA((m - 1, C)),
            pltpu.SemaphoreType.DMA((Z,)),
            pltpu.SemaphoreType.DMA((Z,)),
        ],
        compiler_params=pltpu.CompilerParams(
            collective_id=0, has_side_effects=True, vmem_limit_bytes=VMEM_BYTES - size
        ),
    )(up, down, pup, pdown, slope_norm, slope_bias, pnorm, pbias)
    half_up, half_down, half_norm, half_bias, new_up, new_down, next_norm, next_bias = pl.pallas_call(
        put_kernel,
        out_shape=(
            jax.ShapeDtypeStruct((Z, 2, CH, R, L), BF16),
            jax.ShapeDtypeStruct((L, n * rows), BF16),
            jax.ShapeDtypeStruct((width,), BF16),
            jax.ShapeDtypeStruct((width,), BF16),
            jax.ShapeDtypeStruct((CH, R, L), F32),
            jax.ShapeDtypeStruct((CH, R, L), F32),
            jax.ShapeDtypeStruct((rows,), F32),
            jax.ShapeDtypeStruct((rows,), F32),
        ),
        in_specs=[vmem] * 4,
        out_specs=(hbm, hbm, vmem, vmem, hbm, hbm, vmem, vmem),
        scratch_shapes=[pltpu.SemaphoreType.DMA((4 * Z + 2,))],
        compiler_params=pltpu.CompilerParams(vmem_limit_bytes=1 << 20),
    )(*(pltpu.with_memory_space_constraint(x, pltpu.VMEM) for x in (G, T, NX, sums)))
    half_up = half_up.reshape(n * rows, L)
    next_up = new_up.reshape(rows, L)
    next_down = new_down.reshape(rows, L).T
    return (half_up, half_down, half_norm, half_bias, next_up, next_down, next_norm, next_bias)


def solution(mesh):
    return jax.shard_map(
        on_device,
        mesh=mesh,
        in_specs=(
            P(("ens", "batch"), None, "cols"),
            P(("ens", "batch"), "cols", None),
            P(("ens", "batch"), None),
            P(("ens", "batch"), None),
            P(("ens", "batch"), "cols"),
            P(("ens", "cols"), "batch"),
            P(("ens", "batch")),
            P(("ens", "batch")),
        ),
        out_specs=(
            P("ens", "cols"),
            P(("ens", "cols"), None),
            P("ens"),
            P("ens"),
            P(("ens", "batch"), "cols"),
            P(("ens", "cols"), "batch"),
            P(("ens", "batch")),
            P(("ens", "batch")),
        ),
        check_vma=False,
    )
```

```python
import functools
import math

import jax
import jax.numpy as jnp
from jax import lax
from jax.experimental import pallas as pl
from jax.experimental.pallas import tpu as pltpu
from jax.sharding import PartitionSpec as P

learn_rate = 0.4
MESH = pl.DeviceIdType.MESH
R = 8
LANE = 128
SPLIT = 0.6
HEAD, TAIL = 1, 2
DEPTH = 4
SENDS = 2
VMEM_BYTES = 66_000_000
F32, BF16 = jnp.float32, jnp.bfloat16


def kernel(
    n,
    m,
    LA,
    up_ref,
    down_ref,
    pup_ref,
    pdown_ref,
    norm_ref,
    bias_ref,
    pnorm_ref,
    pbias_ref,
    G,
    T,
    NX,
    half_norm_ref,
    half_bias_ref,
    next_norm_ref,
    next_bias_ref,
    stage,
    turn,
    XA,
    XB,
    RYA,
    RYB,
    RZA,
    RZB,
    PR,
    SQ,
    V,
    VP,
    VY,
    VZ,
    up_sem,
    down_sem,
    par_sem,
    send,
    recv,
    sum_recv,
    gather_recv,
    gather_send,
    sq_send,
    sq_recv,
    v_send,
    v_recv,
):
    Z = n // 2
    C = NX.shape[0]
    CH = C // 2
    H0 = CH // 2
    L = NX.shape[2]
    me = lax.axis_index("batch")
    core = lax.axis_index("cols")
    z = me // 2
    y = me % 2
    other = z * 2 + 1 - y
    rate = n ** (-0.5)

    def slot(p):
        return jnp.where(p < H0, p, jnp.where(p < H0 + CH, p - H0 + CH, p - CH))

    def load_up(c):
        return pltpu.make_async_copy(up_ref.at[:, :, c], stage.at[c % 2], up_sem.at[c % 2])

    blocks = L // LANE
    share = -(-blocks // H0)
    back = -(-blocks // (CH - H0))

    def load_down(b):
        return pltpu.make_async_copy(
            down_ref.at[pl.ds(b * LANE, LANE)], turn.at[b % DEPTH], down_sem.at[b % DEPTH]
        )

    def turn_block(b):
        def pieces(store):
            for j in range(n * CH * R // LANE):
                tile = turn[b % DEPTH, :, j * LANE : (j + 1) * LANE].T
                for i in range(LANE // R):
                    piece = j * (LANE // R) + i
                    d, k = piece // CH, piece % CH
                    store(d // 2, d % 2, CH + k, tile[i * R : (i + 1) * R].astype(BF16))

        @pl.when(b * LANE < LA)
        def _():
            at = pl.ds(pl.multiple_of(b * LANE, LANE), LANE)

            def store(d, v, c, x):
                XA[c, v, d, :, at] = x

            pieces(store)

        @pl.when(b * LANE >= LA)
        def _():
            at = pl.ds(pl.multiple_of(b * LANE - LA, LANE), LANE)

            def store(d, v, c, x):
                XB[c, d, v, :, at] = x

            pieces(store)

    def load_params():
        return [
            pltpu.make_async_copy(pup_ref, PR.at[pl.ds(0, CH)], par_sem.at[0]),
            pltpu.make_async_copy(pdown_ref, PR.at[pl.ds(CH, CH)], par_sem.at[1]),
        ]

    def load_vectors():
        return [
            pltpu.make_async_copy(norm_ref, V.at[0], par_sem.at[2]),
            pltpu.make_async_copy(bias_ref, V.at[1], par_sem.at[3]),
            pltpu.make_async_copy(pnorm_ref, VP.at[0], par_sem.at[4]),
            pltpu.make_async_copy(pbias_ref, VP.at[1], par_sem.at[5]),
        ]

    load_up(0).start()
    for d in load_params() + load_vectors():
        d.start()

    for b in range(min(DEPTH - 1, blocks)):
        load_down(b).start()

    barrier = pltpu.get_barrier_semaphore()
    def greet(to):
        pl.semaphore_signal(barrier, inc=1, device_id={"batch": to}, device_id_type=MESH)

    greet(other)

    @pl.when(z > 0)
    def _():
        greet(me - 2)

    @pl.when(z < Z - 1)
    def _():
        greet(me + 2)

    for o in range(1, m):
        pl.semaphore_signal(
            barrier, inc=1, device_id={"cols": (core + o) % m}, device_id_type=MESH
        )
    pl.semaphore_wait(barrier, jnp.where((z == 0) | (z == Z - 1), m + 1, m + 2))

    waits = recv.shape[1]

    def remote(src, dst, kind, p, to):
        return pltpu.make_async_remote_copy(
            src_ref=src,
            dst_ref=dst,
            send_sem=send.at[kind, p % SENDS],
            recv_sem=recv.at[kind, p % waits],
            device_id={"batch": to},
            device_id_type=MESH,
        )

    def free(copy, p):
        @pl.when(p >= SENDS)
        def _():
            copy(p - SENDS).wait_send()

    def go(copy, p):
        free(copy, p)
        copy(p).start()

    def vec_y():
        return pltpu.make_async_remote_copy(
            src_ref=VZ.at[z],
            dst_ref=VY,
            send_sem=v_send.at[0],
            recv_sem=v_recv.at[0],
            device_id={"batch": other},
            device_id_type=MESH,
        )

    def vec_z(side, lo, count, to):
        ref = VZ.at[pl.ds(lo, count)]
        return pltpu.make_async_remote_copy(
            src_ref=ref,
            dst_ref=ref,
            send_sem=v_send.at[side],
            recv_sem=v_recv.at[side],
            device_id={"batch": to},
            device_id_type=MESH,
        )

    def vec_right(k):
        return vec_z(1, 0, k + 1, jnp.minimum(me + 2, n - 1))

    def vec_left(k):
        return vec_z(2, k, Z - k, jnp.maximum(me - 2, 0))

    def vec_step(t):
        for k in range(Z):

            @pl.when((z == k) & (t == k))
            def _():
                if k > 0:
                    vec_right(k - 1).wait_recv()
                if k < Z - 1:
                    vec_right(k).start()

            @pl.when((z == k) & (t == Z - 1 - k))
            def _():
                if k < Z - 1:
                    vec_left(k + 1).wait_recv()
                if k > 0:
                    vec_left(k).start()

            @pl.when((z == k) & (t == Z))
            def _():
                if k < Z - 1:
                    vec_right(k).wait_send()
                if k > 0:
                    vec_left(k).wait_send()

        @pl.when(t == Z)
        def _():
            total = VZ[0]
            for k in range(1, Z):
                total = total + VZ[k]
            width = VZ.shape[2]
            rows = width // n
            whole = total[2:4] - learn_rate * (total[0:2] * rate)
            halves = whole.astype(BF16)
            half_norm_ref[...] = halves[0:1].reshape(width)
            half_bias_ref[...] = halves[1:2].reshape(width)
            own = pltpu.roll(whole, (n - me) % n * rows, 1)[:, :rows]
            next_norm_ref[...] = own[0:1].reshape(rows)
            next_bias_ref[...] = own[1:2].reshape(rows)

    def sq_copy(p, o):
        return pltpu.make_async_remote_copy(
            src_ref=SQ.at[slot(p), 0],
            dst_ref=SQ.at[slot(p), o],
            send_sem=sq_send.at[o - 1, p % SENDS],
            recv_sem=sq_recv.at[o - 1, p % waits],
            device_id={"cols": (core + o) % m},
            device_id_type=MESH,
        )

    YA, YB, RA, LFA, RB, LFB, GYA, GYB, GRA, GLA, GRB, GLB = range(12)

    def ya(p):
        c = slot(p)
        return remote(XA.at[c, 1 - y], RYA.at[c], YA, p, other)

    def yb(p):
        c = slot(p)
        return remote(XB.at[c, z, 1 - y], RYB.at[c], YB, p, other)

    def gya(p):
        ref = G.at[:, y, slot(p), :, pl.ds(0, LA)]
        return remote(ref, ref, GYA, p, other)

    def gya_in(p):
        ref = G.at[:, 1 - y, slot(p), :, pl.ds(0, LA)]
        return remote(ref, ref, GYA, p, other)

    def gyb(p):
        ref = G.at[z, y, slot(p), :, pl.ds(LA, L - LA)]
        return remote(ref, ref, GYB, p, other)

    def gyb_in(p):
        ref = G.at[z, 1 - y, slot(p), :, pl.ds(LA, L - LA)]
        return remote(ref, ref, GYB, p, other)

    def head(p):
        return p < HEAD

    def tail(p):
        return p >= C - TAIL

    def right_of():
        return jnp.minimum(me + 2, n - 1)

    def left_of():
        return jnp.maximum(me - 2, 0)

    def piece(src, dst, send_sem, recv_sem, to):
        return pltpu.make_async_remote_copy(
            src_ref=src,
            dst_ref=dst,
            send_sem=send_sem,
            recv_sem=recv_sem,
            device_id={"batch": to},
            device_id_type=MESH,
        )

    def sum_piece(first, right, p, d):
        c = slot(p)
        rz = RZA if first else RZB
        kind = (RA if first else RB) if right else (LFA if first else LFB)
        return piece(
            XA.at[c, y, d] if first else XB.at[c, d],
            rz.at[c, d + 1 if right else d],
            send.at[kind, p % SENDS],
            sum_recv.at[2 * first + right, p, d],
            right_of() if right else left_of(),
        )

    def gather_piece(first, right, p, d):
        kind = (GRA if first else GRB) if right else (GLA if first else GLB)
        if first:
            ref = G.at[d, y, slot(p), :, pl.ds(0, LA)]
        else:
            ref = G.at[d, :, slot(p), :, pl.ds(LA, L - LA)]
        return piece(
            ref,
            ref,
            send.at[kind, p % SENDS],
            gather_recv.at[2 * first + right, p - (C - TAIL), d],
            right_of() if right else left_of(),
        )

    def gya_piece(p, d, v):
        ref = G.at[d, v, slot(p), :, pl.ds(0, LA)]
        e = p - (C - TAIL)
        return piece(ref, ref, gather_send.at[e, d], gather_recv.at[4, e, d], other)

    def x_ref(first, c):
        return XA.at[c, y] if first else XB.at[c]

    def sum_right(first, p, k):
        c = slot(p)
        rz = RZA if first else RZB
        return remote(
            x_ref(first, c).at[pl.ds(k + 1, Z - 1 - k)],
            rz.at[c, pl.ds(k + 2, Z - 1 - k)],
            RA if first else RB,
            p,
            right_of(),
        )

    def sum_left(first, p, k):
        c = slot(p)
        rz = RZA if first else RZB
        return remote(
            x_ref(first, c).at[pl.ds(0, k)],
            rz.at[c, pl.ds(0, k)],
            LFA if first else LFB,
            p,
            left_of(),
        )

    def add(first, p, lo, count, at):
        c = slot(p)
        rz = RZA if first else RZB
        for d in range(count):
            if first:
                XA[c, y, lo + d] = (
                    XA[c, y, lo + d].astype(F32) + rz[c, at + d].astype(F32)
                ).astype(BF16)
            else:
                XB[c, lo + d] = (
                    XB[c, lo + d].astype(F32) + rz[c, at + d].astype(F32)
                ).astype(BF16)

    def at_hop(t, k, bulk, pieces, special):
        for right in (True, False):
            p = t - k if right else t - (Z - 1 - k)
            here = (z == k) & (p >= 0) & (p < C)

            @pl.when(here & jnp.logical_not(special(p)))
            def _():
                bulk(right, p)

            @pl.when(here & special(p))
            def _():
                pieces(right, p)

    def reduce_step(first, t):
        for k in range(Z):

            def to_right(p):
                return sum_right(first, p, k)

            def to_left(p):
                return sum_left(first, p, k)

            def bulk(right, p):
                if right:
                    if k > 0:
                        sum_right(first, p, k - 1).wait_recv()
                        add(first, p, k, Z - k, k + 1)
                    if k < Z - 1:
                        go(to_right, p)
                else:
                    if k < Z - 1:
                        sum_left(first, p, k + 1).wait_recv()
                        add(first, p, 0, k + 1, 0)
                    if k > 0:
                        go(to_left, p)

            def pieces(right, p):
                if k < Z - 1 if right else k > 0:
                    free(to_right if right else to_left, p)
                for d in range(Z - 1, k - 1, -1) if right else range(k + 1):
                    if k > 0 if right else k < Z - 1:
                        sum_piece(first, right, p, d).wait_recv()
                        add(first, p, d, 1, d + 1 if right else d)
                    if d != k:
                        sum_piece(first, right, p, d).start()

            at_hop(t, k, bulk, pieces, head)

    def g_ref(first, c, lo, count):
        at = pl.ds(lo, count)
        if first:
            return G.at[at, y, c, :, pl.ds(0, LA)]
        return G.at[at, :, c, :, pl.ds(LA, L - LA)]

    def gather_right(first, p, k):
        ref = g_ref(first, slot(p), 0, k + 1)
        return remote(ref, ref, GRA if first else GRB, p, right_of())

    def gather_left(first, p, k):
        ref = g_ref(first, slot(p), k, Z - k)
        return remote(ref, ref, GLA if first else GLB, p, left_of())

    def gather_step(first, t):
        for k in range(Z):

            def to_right(p):
                return gather_right(first, p, k)

            def to_left(p):
                return gather_left(first, p, k)

            def bulk(right, p):
                if right:
                    if k > 0:
                        gather_right(first, p, k - 1).wait_recv()
                    if k < Z - 1:
                        go(to_right, p)
                else:
                    if k < Z - 1:
                        gather_left(first, p, k + 1).wait_recv()
                    if k > 0:
                        go(to_left, p)

            def pieces(right, p):
                on = k < Z - 1 if right else k > 0
                if on:
                    free(to_right if right else to_left, p)
                for d in range(k, -1, -1) if right else range(k, Z):
                    if d != k:
                        gather_piece(first, right, p, d).wait_recv()
                    if on:
                        gather_piece(first, right, p, d).start()
                    if first and d != k:
                        gya_piece(p, d, y).start()

            at_hop(t, k, bulk, pieces, tail)

    def last_sends(p):
        for copy in (ya, yb, gyb):
            copy(p).wait_send()
        for o in range(1, m):
            sq_copy(p, o).wait_send()
        for k in range(Z):

            @pl.when(z == k)
            def _():
                for first in (True, False):
                    if k < Z - 1:
                        sum_right(first, p, k).wait_send()
                        gather_right(first, p, k).wait_send()
                    if k > 0:
                        sum_left(first, p, k).wait_send()
                        gather_left(first, p, k).wait_send()

    def back_block(b):
        at = pl.ds(pl.multiple_of(b * LANE, LANE), LANE)
        for j in range(n * CH * R // LANE):
            rows = []
            for i in range(LANE // R):
                piece = j * (LANE // R) + i
                d, k = piece // CH, piece % CH
                rows.append(G[d // 2, d % 2, CH + k, :, at].astype(F32))
            tile = jnp.concatenate(rows, axis=0)
            T[at, j * LANE : (j + 1) * LANE] = tile.T.astype(BF16)

    def lanes(x):
        s = x[:, :LANE] * x[:, :LANE]
        for i in range(1, L // LANE):
            part = x[:, i * LANE : (i + 1) * LANE]
            s = s + part * part
        return s

    def when_chunk(c):
        return pl.when((c >= 0) & (c < C))

    @pl.loop(0, C + 2 * Z)
    def _(t):
        def load_at(p, act):
            @pl.when((p < H0) | ((p >= H0 + CH) & (p < C)))
            def _():
                act(slot(p))

        load_at(t + 1, lambda c: load_up(c).start())

        def cast(c):
            load_up(c).wait()
            for d in range(Z):
                for v in range(2):
                    XA[c, v, d] = stage[c % 2, d, v, :, :LA].astype(BF16)
                    XB[c, d, v] = stage[c % 2, d, v, :, LA:].astype(BF16)

        load_at(t, cast)

        @pl.when(t < C)
        def _():
            go(ya, t)

        reduce_step(False, t)
        s = t - 1

        @pl.when(t == 0)
        def _():
            for d in load_vectors():
                d.wait()
            width = VY.shape[1]
            place = jnp.zeros((1, width - VP.shape[2]), F32)
            for i in range(2):
                VZ[z, i : i + 1] = V[i]
                own = jnp.concatenate([VP[i], place], axis=1)
                VZ[z, 2 + i : 3 + i] = pltpu.roll(own, me * VP.shape[2], 1)
            vec_y().start()

        @pl.when(t == 1)
        def _():
            vec_y().wait()
            VZ[z] = VZ[z] + VY[...]

        @when_chunk(s)
        def _():
            c = slot(s)
            ya(s).wait_recv()
            for d in range(Z):
                XA[c, y, d] = (XA[c, y, d].astype(F32) + RYA[c, d].astype(F32)).astype(BF16)

        reduce_step(True, s)
        b = t - (Z - 1)

        @when_chunk(b)
        def _():
            go(yb, b)

        u = t - Z

        @pl.when(u == 0)
        def _():
            for d in load_params():
                d.wait()

        @when_chunk(u)
        def _():
            f = slot(u)
            yb(u).wait_recv()
            NX[f, :, :LA] = XA[f, y, z].astype(F32) * rate
            NX[f, :, LA:] = (XB[f, z, y].astype(F32) + RYB[f].astype(F32)) * rate
            SQ[f, 0, 0] = lanes(NX[f])
            SQ[f, 0, 1] = lanes(PR[f])
            for o in range(1, m):
                go(lambda p, o=o: sq_copy(p, o), u)

        @when_chunk(u - 1)
        def _():
            gyb_in(u - 1).wait_recv()

        gather_step(False, u - 1)
        e = u - Z

        @when_chunk(u)
        def _():
            f = slot(u)
            for o in range(1, m):
                sq_copy(u, o).wait_recv()
            g = SQ[f, 0, 0]
            p = SQ[f, 0, 1]
            for o in range(1, m):
                g = g + SQ[f, o, 0]
                p = p + SQ[f, o, 1]
            g = jnp.sum(g, axis=1, keepdims=True)
            p = jnp.sum(p, axis=1, keepdims=True)
            scale = learn_rate * (jnp.sqrt(p) * lax.rsqrt(g + 1e-06))
            new = PR[f] - NX[f] * scale
            NX[f] = new
            G[z, y, f] = new.astype(BF16)
            go(gyb, u)

            @pl.when(tail(u))
            def _():
                gya_piece(u, z, y).start()

        gather_step(True, u)

        w = u - (Z - 1)

        @pl.when((w >= 0) & jnp.logical_not(tail(w)))
        def _():
            go(gya, w)

        vec_step(t - 1)

        @pl.when((e >= 0) & jnp.logical_not(tail(e)))
        def _():
            gya_in(e).wait_recv()

        @pl.when((e < C) & tail(e))
        def _():
            for d in range(Z):
                gya_piece(e, d, 1 - y).wait_recv()
                gya_piece(e, d, y).wait_send()

        for i in range(share):
            b = t * share + i

            @pl.when(b + DEPTH - 1 < blocks)
            def _():
                load_down(b + DEPTH - 1).start()

            @pl.when(b < blocks)
            def _():
                load_down(b).wait()
                turn_block(b)

        for i in range(back):
            w = (t - (H0 + CH + 2 * Z)) * back + i

            @pl.when((w >= 0) & (w < blocks))
            def _():
                back_block(w)

    for i in range(SENDS):
        last_sends(C - SENDS + i)
        gya(C - TAIL - SENDS + i).wait_send()


def put_kernel(
    G,
    T,
    NX,
    half_norm,
    half_bias,
    next_norm,
    next_bias,
    half_up_ref,
    half_down_ref,
    half_norm_ref,
    half_bias_ref,
    next_up_ref,
    next_down_ref,
    next_norm_ref,
    next_bias_ref,
    sem,
):
    Z = G.shape[0]
    CH = G.shape[2] // 2
    part = T.shape[0] // (2 * Z)
    copies = []

    def put(src, dst):
        d = pltpu.make_async_copy(src, dst, sem.at[len(copies)])
        d.start()
        copies.append(d)

    for k in range(Z):
        for v in range(2):
            put(G.at[k, v, pl.ds(0, CH)], half_up_ref.at[k, v])
            at = pl.ds((2 * k + v) * part, part)
            put(T.at[at], half_down_ref.at[at])
    put(NX.at[pl.ds(0, CH)], next_up_ref)
    put(NX.at[pl.ds(CH, CH)], next_down_ref)
    put(half_norm, half_norm_ref)
    put(half_bias, half_bias_ref)
    put(next_norm, next_norm_ref)
    put(next_bias, next_bias_ref)
    for d in copies:
        d.wait()


def on_device(
    slope_up, slope_down, slope_norm, slope_bias, param_up, param_down, param_norm, param_bias
):
    n = lax.axis_size("batch")
    m = lax.axis_size("cols")
    Z = n // 2
    rows, L = param_up.shape
    CH = rows // R
    C = 2 * CH
    LA = max(1, round(SPLIT * L / LANE)) * LANE
    LB = L - LA
    width = slope_norm.shape[1]
    up = slope_up[0].reshape(Z, 2, CH, R, L)
    down = slope_down[0]
    pup = param_up.reshape(CH, R, L)
    pdown = param_down.T.reshape(CH, R, L)
    pnorm = param_norm.reshape(1, rows)
    pbias = param_bias.reshape(1, rows)
    hbm = pl.BlockSpec(memory_space=pl.ANY)
    vmem = pl.BlockSpec(memory_space=pltpu.VMEM)
    kept = [((Z, 2, C, R, L), BF16), ((L, n * rows), BF16), ((C, R, L), F32)]
    kept += [((width,), BF16)] * 2 + [((rows,), F32)] * 2
    size = sum(jnp.dtype(dtype).itemsize * math.prod(shape) for shape, dtype in kept)
    held = pl.pallas_call(
        functools.partial(kernel, n, m, LA),
        out_shape=tuple(pltpu.VMEM(shape, dtype) for shape, dtype in kept),
        in_specs=[hbm] * 8,
        out_specs=(vmem,) * 7,
        scratch_shapes=[
            pltpu.VMEM((2, Z, 2, R, L), F32),
            pltpu.VMEM((DEPTH, LANE, n * rows), F32),
            pltpu.VMEM((C, 2, Z, R, LA), BF16),
            pltpu.VMEM((C, Z, 2, R, LB), BF16),
            pltpu.VMEM((C, Z, R, LA), BF16),
            pltpu.VMEM((C, R, LB), BF16),
            pltpu.VMEM((C, Z + 1, R, LA), BF16),
            pltpu.VMEM((C, Z + 1, 2, R, LB), BF16),
            pltpu.VMEM((C, R, L), F32),
            pltpu.VMEM((C, m, 2, R, LANE), F32),
            pltpu.VMEM((2, 1, width), F32),
            pltpu.VMEM((2, 1, rows), F32),
            pltpu.VMEM((4, width), F32),
            pltpu.VMEM((Z, 4, width), F32),
            pltpu.SemaphoreType.DMA((2,)),
            pltpu.SemaphoreType.DMA((DEPTH,)),
            pltpu.SemaphoreType.DMA((6,)),
            pltpu.SemaphoreType.DMA((12, SENDS)),
            pltpu.SemaphoreType.DMA((12, Z + 2)),
            pltpu.SemaphoreType.DMA((4, HEAD, Z)),
            pltpu.SemaphoreType.DMA((5, TAIL, Z)),
            pltpu.SemaphoreType.DMA((TAIL, Z)),
            pltpu.SemaphoreType.DMA((m - 1, SENDS)),
            pltpu.SemaphoreType.DMA((m - 1, Z + 2)),
            pltpu.SemaphoreType.DMA((3,)),
            pltpu.SemaphoreType.DMA((3,)),
        ],
        compiler_params=pltpu.CompilerParams(
            collective_id=0, has_side_effects=True, vmem_limit_bytes=VMEM_BYTES - size
        ),
    )(up, down, pup, pdown, slope_norm, slope_bias, pnorm, pbias)
    half_up, half_down, half_norm, half_bias, new_up, new_down, next_norm, next_bias = pl.pallas_call(
        put_kernel,
        out_shape=(
            jax.ShapeDtypeStruct((Z, 2, CH, R, L), BF16),
            jax.ShapeDtypeStruct((L, n * rows), BF16),
            jax.ShapeDtypeStruct((width,), BF16),
            jax.ShapeDtypeStruct((width,), BF16),
            jax.ShapeDtypeStruct((CH, R, L), F32),
            jax.ShapeDtypeStruct((CH, R, L), F32),
            jax.ShapeDtypeStruct((rows,), F32),
            jax.ShapeDtypeStruct((rows,), F32),
        ),
        in_specs=[vmem] * 7,
        out_specs=(hbm,) * 8,
        scratch_shapes=[pltpu.SemaphoreType.DMA((4 * Z + 6,))],
        compiler_params=pltpu.CompilerParams(vmem_limit_bytes=1 << 20),
    )(*(pltpu.with_memory_space_constraint(x, pltpu.VMEM) for x in held))
    half_up = half_up.reshape(n * rows, L)
    next_up = new_up.reshape(rows, L)
    next_down = new_down.reshape(rows, L).T
    return (half_up, half_down, half_norm, half_bias, next_up, next_down, next_norm, next_bias)


def solution(mesh):
    return jax.shard_map(
        on_device,
        mesh=mesh,
        in_specs=(
            P(("ens", "batch"), None, "cols"),
            P(("ens", "batch"), "cols", None),
            P(("ens", "batch"), None),
            P(("ens", "batch"), None),
            P(("ens", "batch"), "cols"),
            P(("ens", "cols"), "batch"),
            P(("ens", "batch")),
            P(("ens", "batch")),
        ),
        out_specs=(
            P("ens", "cols"),
            P(("ens", "cols"), None),
            P("ens"),
            P("ens"),
            P(("ens", "batch"), "cols"),
            P(("ens", "cols"), "batch"),
            P(("ens", "batch")),
            P(("ens", "batch")),
        ),
        check_vma=False,
    )
```

```python
import functools
import math

import jax
import jax.numpy as jnp
from jax import lax
from jax.experimental import pallas as pl
from jax.experimental.pallas import tpu as pltpu
from jax.sharding import PartitionSpec as P

learn_rate = 0.4
MESH = pl.DeviceIdType.MESH
R = 8
LANE = 128
SPLIT = 0.6
HEAD, TAIL = 1, 1
DEPTH = 4
SENDS = 2
LAST, LAST_SPLIT = 6, 0.75
VMEM_BYTES = 66_000_000
F32, BF16 = jnp.float32, jnp.bfloat16


def kernel(
    n,
    m,
    LA,
    LW,
    up_ref,
    down_ref,
    pup_ref,
    pdown_ref,
    norm_ref,
    bias_ref,
    pnorm_ref,
    pbias_ref,
    G,
    T,
    NX,
    half_norm_ref,
    half_bias_ref,
    next_norm_ref,
    next_bias_ref,
    stage,
    turn,
    XA,
    XB,
    RYA,
    RYB,
    RZA,
    RZB,
    PR,
    SQ,
    V,
    VP,
    VY,
    VZ,
    up_sem,
    down_sem,
    par_sem,
    send,
    recv,
    first_recv,
    sum_recv,
    gather_recv,
    gather_send,
    sq_send,
    sq_recv,
    v_send,
    v_recv,
):
    Z = n // 2
    C = NX.shape[0]
    CH = C // 2
    H0 = CH // 2
    L = NX.shape[2]
    me = lax.axis_index("batch")
    core = lax.axis_index("cols")
    z = me // 2
    y = me % 2
    other = z * 2 + 1 - y
    rate = n ** (-0.5)

    def slot(p):
        return jnp.where(p < H0, p, jnp.where(p < H0 + CH, p - H0 + CH, p - CH))

    def load_up(c):
        return pltpu.make_async_copy(up_ref.at[:, :, c], stage.at[c % 2], up_sem.at[c % 2])

    blocks = L // LANE
    share = -(-blocks // H0)
    back = -(-blocks // (CH - H0))

    def load_down(b):
        return pltpu.make_async_copy(
            down_ref.at[pl.ds(b * LANE, LANE)], turn.at[b % DEPTH], down_sem.at[b % DEPTH]
        )

    def turn_block(b):
        def pieces(store):
            for j in range(n * CH * R // LANE):
                tile = turn[b % DEPTH, :, j * LANE : (j + 1) * LANE].T
                for i in range(LANE // R):
                    piece = j * (LANE // R) + i
                    d, k = piece // CH, piece % CH
                    store(d // 2, d % 2, CH + k, tile[i * R : (i + 1) * R].astype(BF16))

        @pl.when(b * LANE < LA)
        def _():
            at = pl.ds(pl.multiple_of(b * LANE, LANE), LANE)

            def store(d, v, c, x):
                XA[c, v, d, :, at] = x

            pieces(store)

        @pl.when(b * LANE >= LA)
        def _():
            at = pl.ds(pl.multiple_of(b * LANE - LA, LANE), LANE)

            def store(d, v, c, x):
                XB[c, d, v, :, at] = x

            pieces(store)

    def load_params():
        return [
            pltpu.make_async_copy(pup_ref, PR.at[pl.ds(0, CH)], par_sem.at[0]),
            pltpu.make_async_copy(pdown_ref, PR.at[pl.ds(CH, CH)], par_sem.at[1]),
        ]

    def load_vectors():
        return [
            pltpu.make_async_copy(norm_ref, V.at[0], par_sem.at[2]),
            pltpu.make_async_copy(bias_ref, V.at[1], par_sem.at[3]),
            pltpu.make_async_copy(pnorm_ref, VP.at[0], par_sem.at[4]),
            pltpu.make_async_copy(pbias_ref, VP.at[1], par_sem.at[5]),
        ]

    load_up(0).start()
    for d in load_params() + load_vectors():
        d.start()

    for b in range(min(DEPTH - 1, blocks)):
        load_down(b).start()

    barrier = pltpu.get_barrier_semaphore()
    def greet(to):
        pl.semaphore_signal(barrier, inc=1, device_id={"batch": to}, device_id_type=MESH)

    greet(other)

    @pl.when(z > 0)
    def _():
        greet(me - 2)

    @pl.when(z < Z - 1)
    def _():
        greet(me + 2)

    for o in range(1, m):
        pl.semaphore_signal(
            barrier, inc=1, device_id={"cols": (core + o) % m}, device_id_type=MESH
        )
    pl.semaphore_wait(barrier, jnp.where((z == 0) | (z == Z - 1), m + 1, m + 2))

    waits = recv.shape[1]

    def remote(src, dst, kind, p, to):
        return pltpu.make_async_remote_copy(
            src_ref=src,
            dst_ref=dst,
            send_sem=send.at[kind, p % SENDS],
            recv_sem=recv.at[kind, p % waits],
            device_id={"batch": to},
            device_id_type=MESH,
        )

    def free(copy, p):
        @pl.when(p >= SENDS)
        def _():
            copy(p - SENDS).wait_send()

    def go(copy, p):
        free(copy, p)
        copy(p).start()

    def wide(p):
        return p >= C - LAST

    def split(p, act):
        @pl.when(jnp.logical_not(wide(p)))
        def _():
            act(LA)

        @pl.when(wide(p))
        def _():
            act(LW)

    def free_split(copy, p):
        @pl.when(p >= SENDS)
        def _():
            split(p - SENDS, lambda la: copy(p - SENDS, la).wait_send())

    def go_split(copy, p):
        free_split(copy, p)
        split(p, lambda la: copy(p, la).start())

    def vec_y():
        return pltpu.make_async_remote_copy(
            src_ref=VZ.at[z],
            dst_ref=VY,
            send_sem=v_send.at[0],
            recv_sem=v_recv.at[0],
            device_id={"batch": other},
            device_id_type=MESH,
        )

    def vec_z(side, lo, count, to):
        ref = VZ.at[pl.ds(lo, count)]
        return pltpu.make_async_remote_copy(
            src_ref=ref,
            dst_ref=ref,
            send_sem=v_send.at[side],
            recv_sem=v_recv.at[side],
            device_id={"batch": to},
            device_id_type=MESH,
        )

    def vec_right(k):
        return vec_z(1, 0, k + 1, jnp.minimum(me + 2, n - 1))

    def vec_left(k):
        return vec_z(2, k, Z - k, jnp.maximum(me - 2, 0))

    def vec_step(t):
        for k in range(Z):

            @pl.when((z == k) & (t == k))
            def _():
                if k > 0:
                    vec_right(k - 1).wait_recv()
                if k < Z - 1:
                    vec_right(k).start()

            @pl.when((z == k) & (t == Z - 1 - k))
            def _():
                if k < Z - 1:
                    vec_left(k + 1).wait_recv()
                if k > 0:
                    vec_left(k).start()

            @pl.when((z == k) & (t == Z))
            def _():
                if k < Z - 1:
                    vec_right(k).wait_send()
                if k > 0:
                    vec_left(k).wait_send()

        @pl.when(t == Z)
        def _():
            total = VZ[0]
            for k in range(1, Z):
                total = total + VZ[k]
            width = VZ.shape[2]
            rows = width // n
            whole = total[2:4] - learn_rate * (total[0:2] * rate)
            halves = whole.astype(BF16)
            half_norm_ref[...] = halves[0:1].reshape(width)
            half_bias_ref[...] = halves[1:2].reshape(width)
            own = pltpu.roll(whole, (n - me) % n * rows, 1)[:, :rows]
            next_norm_ref[...] = own[0:1].reshape(rows)
            next_bias_ref[...] = own[1:2].reshape(rows)

    def sq_copy(p, o):
        return pltpu.make_async_remote_copy(
            src_ref=SQ.at[slot(p), 0],
            dst_ref=SQ.at[slot(p), o],
            send_sem=sq_send.at[o - 1, p % SENDS],
            recv_sem=sq_recv.at[o - 1, p % waits],
            device_id={"cols": (core + o) % m},
            device_id_type=MESH,
        )

    YA, YB, RA, LFA, RB, LFB, GYA, GYB, GRA, GLA, GRB, GLB = range(12)

    def ya(p):
        c = slot(p)
        return remote(XA.at[c, 1 - y], RYA.at[c], YA, p, other)

    def yb(p):
        c = slot(p)
        return remote(XB.at[c, z, 1 - y], RYB.at[c], YB, p, other)

    def gya(p, la):
        ref = G.at[:, y, slot(p), :, pl.ds(0, la)]
        return remote(ref, ref, GYA, p, other)

    def gya_in(p, la):
        ref = G.at[:, 1 - y, slot(p), :, pl.ds(0, la)]
        return remote(ref, ref, GYA, p, other)

    def gyb(p, la):
        ref = G.at[z, y, slot(p), :, pl.ds(la, L - la)]
        return remote(ref, ref, GYB, p, other)

    def gyb_in(p, la):
        ref = G.at[z, 1 - y, slot(p), :, pl.ds(la, L - la)]
        return remote(ref, ref, GYB, p, other)

    def head(p):
        return p < HEAD

    def tail(p):
        return p >= C - TAIL

    def right_of():
        return jnp.minimum(me + 2, n - 1)

    def left_of():
        return jnp.maximum(me - 2, 0)

    def piece(src, dst, send_sem, recv_sem, to):
        return pltpu.make_async_remote_copy(
            src_ref=src,
            dst_ref=dst,
            send_sem=send_sem,
            recv_sem=recv_sem,
            device_id={"batch": to},
            device_id_type=MESH,
        )

    def ya_piece(p, d):
        c = slot(p)
        return piece(
            XA.at[c, 1 - y, d],
            RYA.at[c, d],
            send.at[YA, p % SENDS],
            first_recv.at[p, d],
            other,
        )

    def take(p, d):
        c = slot(p)
        ya_piece(p, d).wait_recv()
        XA[c, y, d] = (XA[c, y, d].astype(F32) + RYA[c, d].astype(F32)).astype(BF16)

    inward = [d for i in range(Z // 2) for d in (Z - 1 - i, i)]

    def sum_piece(first, right, p, d):
        c = slot(p)
        rz = RZA if first else RZB
        kind = (RA if first else RB) if right else (LFA if first else LFB)
        return piece(
            XA.at[c, y, d] if first else XB.at[c, d],
            rz.at[c, d + 1 if right else d],
            send.at[kind, p % SENDS],
            sum_recv.at[2 * first + right, p, d],
            right_of() if right else left_of(),
        )

    def gather_piece(first, right, p, d):
        kind = (GRA if first else GRB) if right else (GLA if first else GLB)
        if first:
            ref = G.at[d, y, slot(p), :, pl.ds(0, LW)]
        else:
            ref = G.at[d, :, slot(p), :, pl.ds(LW, L - LW)]
        return piece(
            ref,
            ref,
            send.at[kind, p % SENDS],
            gather_recv.at[2 * first + right, p - (C - TAIL), d],
            right_of() if right else left_of(),
        )

    def gya_piece(p, d, v):
        ref = G.at[d, v, slot(p), :, pl.ds(0, LW)]
        e = p - (C - TAIL)
        return piece(ref, ref, gather_send.at[e, d], gather_recv.at[4, e, d], other)

    def x_ref(first, c):
        return XA.at[c, y] if first else XB.at[c]

    def sum_right(first, p, k):
        c = slot(p)
        rz = RZA if first else RZB
        return remote(
            x_ref(first, c).at[pl.ds(k + 1, Z - 1 - k)],
            rz.at[c, pl.ds(k + 2, Z - 1 - k)],
            RA if first else RB,
            p,
            right_of(),
        )

    def sum_left(first, p, k):
        c = slot(p)
        rz = RZA if first else RZB
        return remote(
            x_ref(first, c).at[pl.ds(0, k)],
            rz.at[c, pl.ds(0, k)],
            LFA if first else LFB,
            p,
            left_of(),
        )

    def add(first, p, lo, count, at):
        c = slot(p)
        rz = RZA if first else RZB
        for d in range(count):
            if first:
                XA[c, y, lo + d] = (
                    XA[c, y, lo + d].astype(F32) + rz[c, at + d].astype(F32)
                ).astype(BF16)
            else:
                XB[c, lo + d] = (
                    XB[c, lo + d].astype(F32) + rz[c, at + d].astype(F32)
                ).astype(BF16)

    def at_hop(t, k, bulk, pieces, special):
        for right in (True, False):
            p = t - k if right else t - (Z - 1 - k)
            here = (z == k) & (p >= 0) & (p < C)

            @pl.when(here & jnp.logical_not(special(p)))
            def _():
                bulk(right, p)

            @pl.when(here & special(p))
            def _():
                pieces(right, p)

    def reduce_step(first, t):
        for k in range(Z):

            def to_right(p):
                return sum_right(first, p, k)

            def to_left(p):
                return sum_left(first, p, k)

            def bulk(right, p):
                if right:
                    if k > 0:
                        sum_right(first, p, k - 1).wait_recv()
                        add(first, p, k, Z - k, k + 1)
                    if k < Z - 1:
                        go(to_right, p)
                else:
                    if k < Z - 1:
                        sum_left(first, p, k + 1).wait_recv()
                        add(first, p, 0, k + 1, 0)
                    if k > 0:
                        go(to_left, p)

            def pieces(right, p):
                if k < Z - 1 if right else k > 0:
                    free(to_right if right else to_left, p)
                for d in range(Z - 1, k - 1, -1) if right else range(k + 1):
                    if first and k == (0 if right else Z - 1):
                        take(p, d)
                    if k > 0 if right else k < Z - 1:
                        sum_piece(first, right, p, d).wait_recv()
                        add(first, p, d, 1, d + 1 if right else d)
                    if d != k:
                        sum_piece(first, right, p, d).start()

            at_hop(t, k, bulk, pieces, head)

    def g_ref(first, c, lo, count, la):
        at = pl.ds(lo, count)
        if first:
            return G.at[at, y, c, :, pl.ds(0, la)]
        return G.at[at, :, c, :, pl.ds(la, L - la)]

    def gather_right(first, p, k, la):
        ref = g_ref(first, slot(p), 0, k + 1, la)
        return remote(ref, ref, GRA if first else GRB, p, right_of())

    def gather_left(first, p, k, la):
        ref = g_ref(first, slot(p), k, Z - k, la)
        return remote(ref, ref, GLA if first else GLB, p, left_of())

    def gather_step(first, t):
        for k in range(Z):

            def to_right(p, la):
                return gather_right(first, p, k, la)

            def to_left(p, la):
                return gather_left(first, p, k, la)

            def bulk(right, p):
                if right:
                    if k > 0:
                        split(p, lambda la: gather_right(first, p, k - 1, la).wait_recv())
                    if k < Z - 1:
                        go_split(to_right, p)
                else:
                    if k < Z - 1:
                        split(p, lambda la: gather_left(first, p, k + 1, la).wait_recv())
                    if k > 0:
                        go_split(to_left, p)

            def pieces(right, p):
                on = k < Z - 1 if right else k > 0
                if on:
                    free_split(to_right if right else to_left, p)
                for d in range(k, -1, -1) if right else range(k, Z):
                    if d != k:
                        gather_piece(first, right, p, d).wait_recv()
                    if on:
                        gather_piece(first, right, p, d).start()
                    if first and d != k:
                        gya_piece(p, d, y).start()

            at_hop(t, k, bulk, pieces, tail)

    def last_sends(p):
        for copy in (ya(p), yb(p), gyb(p, LW)):
            copy.wait_send()
        for o in range(1, m):
            sq_copy(p, o).wait_send()
        for k in range(Z):

            @pl.when(z == k)
            def _():
                for first in (True, False):
                    if k < Z - 1:
                        sum_right(first, p, k).wait_send()
                        gather_right(first, p, k, LW).wait_send()
                    if k > 0:
                        sum_left(first, p, k).wait_send()
                        gather_left(first, p, k, LW).wait_send()

    def back_block(b):
        at = pl.ds(pl.multiple_of(b * LANE, LANE), LANE)
        for j in range(n * CH * R // LANE):
            rows = []
            for i in range(LANE // R):
                piece = j * (LANE // R) + i
                d, k = piece // CH, piece % CH
                rows.append(G[d // 2, d % 2, CH + k, :, at].astype(F32))
            tile = jnp.concatenate(rows, axis=0)
            T[at, j * LANE : (j + 1) * LANE] = tile.T.astype(BF16)

    def lanes(x):
        s = x[:, :LANE] * x[:, :LANE]
        for i in range(1, L // LANE):
            part = x[:, i * LANE : (i + 1) * LANE]
            s = s + part * part
        return s

    def when_chunk(c):
        return pl.when((c >= 0) & (c < C))

    def next_block(b):
        @pl.when(b + DEPTH - 1 < blocks)
        def _():
            load_down(b + DEPTH - 1).start()

        load_down(b).wait()
        turn_block(b)

    @pl.loop(0, C + 2 * Z)
    def _(t):
        def load_at(p, act):
            @pl.when((p < H0) | ((p >= H0 + CH) & (p < C)))
            def _():
                act(slot(p))

        load_at(t + 1, lambda c: load_up(c).start())

        def cast(c):
            load_up(c).wait()
            for d in range(Z):
                for v in range(2):
                    XA[c, v, d] = stage[c % 2, d, v, :, :LA].astype(BF16)
                    XB[c, d, v] = stage[c % 2, d, v, :, LA:].astype(BF16)

        load_at(t, cast)

        @pl.when((t < C) & jnp.logical_not(head(t)))
        def _():
            go(ya, t)

        @pl.when(head(t))
        def _():
            free(ya, t)
            for half in range(2):

                @pl.when(z // (Z // 2) == half)
                def _():
                    for d in inward:
                        ya_piece(t, Z - 1 - d if half else d).start()

        reduce_step(False, t)
        s = t - 1

        @pl.when((s >= 0) & head(s) & (z > 0) & (z < Z - 1))
        def _():
            for d in range(Z):
                take(s, d)

        @pl.when((s < C) & jnp.logical_not(head(s)))
        def _():
            c = slot(s)
            ya(s).wait_recv()
            for d in range(Z):
                XA[c, y, d] = (XA[c, y, d].astype(F32) + RYA[c, d].astype(F32)).astype(BF16)

        reduce_step(True, s)
        b = t - (Z - 1)

        @when_chunk(b)
        def _():
            go(yb, b)

        u = t - Z

        @pl.when(u == 0)
        def _():
            for d in load_params():
                d.wait()

        @when_chunk(u)
        def _():
            f = slot(u)
            yb(u).wait_recv()
            NX[f, :, :LA] = XA[f, y, z].astype(F32) * rate
            NX[f, :, LA:] = (XB[f, z, y].astype(F32) + RYB[f].astype(F32)) * rate
            SQ[f, 0, 0] = lanes(NX[f])
            SQ[f, 0, 1] = lanes(PR[f])
            for o in range(1, m):
                go(lambda p, o=o: sq_copy(p, o), u)

        @when_chunk(u - 1)
        def _():
            split(u - 1, lambda la: gyb_in(u - 1, la).wait_recv())

        gather_step(False, u - 1)
        e = u - Z

        @when_chunk(u)
        def _():
            f = slot(u)
            for o in range(1, m):
                sq_copy(u, o).wait_recv()
            g = SQ[f, 0, 0]
            p = SQ[f, 0, 1]
            for o in range(1, m):
                g = g + SQ[f, o, 0]
                p = p + SQ[f, o, 1]
            g = jnp.sum(g, axis=1, keepdims=True)
            p = jnp.sum(p, axis=1, keepdims=True)
            scale = learn_rate * (jnp.sqrt(p) * lax.rsqrt(g + 1e-06))
            new = PR[f] - NX[f] * scale
            NX[f] = new
            G[z, y, f] = new.astype(BF16)
            go_split(gyb, u)

            @pl.when(tail(u))
            def _():
                gya_piece(u, z, y).start()

        gather_step(True, u)

        w = u - (Z - 1)

        @pl.when((w >= 0) & jnp.logical_not(tail(w)))
        def _():
            go_split(gya, w)

        @pl.when(t == 0)
        def _():
            for d in load_vectors():
                d.wait()
            width = VY.shape[1]
            place = jnp.zeros((1, width - VP.shape[2]), F32)
            for i in range(2):
                VZ[z, i : i + 1] = V[i]
                own = jnp.concatenate([VP[i], place], axis=1)
                VZ[z, 2 + i : 3 + i] = pltpu.roll(own, me * VP.shape[2], 1)
            vec_y().start()

        @pl.when(t == 2)
        def _():
            vec_y().wait()
            VZ[z] = VZ[z] + VY[...]

        vec_step(t - 3)

        @pl.when((e >= 0) & jnp.logical_not(tail(e)))
        def _():
            split(e, lambda la: gya_in(e, la).wait_recv())

        @pl.when((e < C) & tail(e))
        def _():
            for d in range(Z):
                gya_piece(e, d, 1 - y).wait_recv()
                gya_piece(e, d, y).wait_send()

        for i in range(share):
            b = t * share + i

            @pl.when(b < blocks)
            def _():
                next_block(b)

        for i in range(back):
            w = (t - (H0 + CH + 2 * Z)) * back + i

            @pl.when((w >= 0) & (w < blocks))
            def _():
                back_block(w)

    for i in range(SENDS):
        last_sends(C - SENDS + i)
        gya(C - TAIL - SENDS + i, LW).wait_send()


def put_kernel(
    G,
    T,
    NX,
    half_norm,
    half_bias,
    next_norm,
    next_bias,
    half_up_ref,
    half_down_ref,
    half_norm_ref,
    half_bias_ref,
    next_up_ref,
    next_down_ref,
    next_norm_ref,
    next_bias_ref,
    sem,
):
    Z = G.shape[0]
    CH = G.shape[2] // 2
    part = T.shape[0] // (2 * Z)
    copies = []

    def put(src, dst):
        d = pltpu.make_async_copy(src, dst, sem.at[len(copies)])
        d.start()
        copies.append(d)

    for k in range(Z):
        for v in range(2):
            put(G.at[k, v, pl.ds(0, CH)], half_up_ref.at[k, v])
            at = pl.ds((2 * k + v) * part, part)
            put(T.at[at], half_down_ref.at[at])
    put(NX.at[pl.ds(0, CH)], next_up_ref)
    put(NX.at[pl.ds(CH, CH)], next_down_ref)
    put(half_norm, half_norm_ref)
    put(half_bias, half_bias_ref)
    put(next_norm, next_norm_ref)
    put(next_bias, next_bias_ref)
    for d in copies:
        d.wait()


def on_device(
    slope_up, slope_down, slope_norm, slope_bias, param_up, param_down, param_norm, param_bias
):
    n = lax.axis_size("batch")
    m = lax.axis_size("cols")
    Z = n // 2
    rows, L = param_up.shape
    CH = rows // R
    C = 2 * CH
    LA = max(1, round(SPLIT * L / LANE)) * LANE
    LB = L - LA
    LW = min(L // LANE - 1, round(LAST_SPLIT * L / LANE)) * LANE
    width = slope_norm.shape[1]
    up = slope_up[0].reshape(Z, 2, CH, R, L)
    down = slope_down[0]
    pup = param_up.reshape(CH, R, L)
    pdown = param_down.T.reshape(CH, R, L)
    pnorm = param_norm.reshape(1, rows)
    pbias = param_bias.reshape(1, rows)
    hbm = pl.BlockSpec(memory_space=pl.ANY)
    vmem = pl.BlockSpec(memory_space=pltpu.VMEM)
    kept = [((Z, 2, C, R, L), BF16), ((L, n * rows), BF16), ((C, R, L), F32)]
    kept += [((width,), BF16)] * 2 + [((rows,), F32)] * 2
    size = sum(jnp.dtype(dtype).itemsize * math.prod(shape) for shape, dtype in kept)
    held = pl.pallas_call(
        functools.partial(kernel, n, m, LA, LW),
        out_shape=tuple(pltpu.VMEM(shape, dtype) for shape, dtype in kept),
        in_specs=[hbm] * 8,
        out_specs=(vmem,) * 7,
        scratch_shapes=[
            pltpu.VMEM((2, Z, 2, R, L), F32),
            pltpu.VMEM((DEPTH, LANE, n * rows), F32),
            pltpu.VMEM((C, 2, Z, R, LA), BF16),
            pltpu.VMEM((C, Z, 2, R, LB), BF16),
            pltpu.VMEM((C, Z, R, LA), BF16),
            pltpu.VMEM((C, R, LB), BF16),
            pltpu.VMEM((C, Z + 1, R, LA), BF16),
            pltpu.VMEM((C, Z + 1, 2, R, LB), BF16),
            pltpu.VMEM((C, R, L), F32),
            pltpu.VMEM((C, m, 2, R, LANE), F32),
            pltpu.VMEM((2, 1, width), F32),
            pltpu.VMEM((2, 1, rows), F32),
            pltpu.VMEM((4, width), F32),
            pltpu.VMEM((Z, 4, width), F32),
            pltpu.SemaphoreType.DMA((2,)),
            pltpu.SemaphoreType.DMA((DEPTH,)),
            pltpu.SemaphoreType.DMA((6,)),
            pltpu.SemaphoreType.DMA((12, SENDS)),
            pltpu.SemaphoreType.DMA((12, Z + 2)),
            pltpu.SemaphoreType.DMA((HEAD, Z)),
            pltpu.SemaphoreType.DMA((4, HEAD, Z)),
            pltpu.SemaphoreType.DMA((5, TAIL, Z)),
            pltpu.SemaphoreType.DMA((TAIL, Z)),
            pltpu.SemaphoreType.DMA((m - 1, SENDS)),
            pltpu.SemaphoreType.DMA((m - 1, Z + 2)),
            pltpu.SemaphoreType.DMA((3,)),
            pltpu.SemaphoreType.DMA((3,)),
        ],
        compiler_params=pltpu.CompilerParams(
            collective_id=0, has_side_effects=True, vmem_limit_bytes=VMEM_BYTES - size
        ),
    )(up, down, pup, pdown, slope_norm, slope_bias, pnorm, pbias)
    half_up, half_down, half_norm, half_bias, new_up, new_down, next_norm, next_bias = pl.pallas_call(
        put_kernel,
        out_shape=(
            jax.ShapeDtypeStruct((Z, 2, CH, R, L), BF16),
            jax.ShapeDtypeStruct((L, n * rows), BF16),
            jax.ShapeDtypeStruct((width,), BF16),
            jax.ShapeDtypeStruct((width,), BF16),
            jax.ShapeDtypeStruct((CH, R, L), F32),
            jax.ShapeDtypeStruct((CH, R, L), F32),
            jax.ShapeDtypeStruct((rows,), F32),
            jax.ShapeDtypeStruct((rows,), F32),
        ),
        in_specs=[vmem] * 7,
        out_specs=(hbm,) * 8,
        scratch_shapes=[pltpu.SemaphoreType.DMA((4 * Z + 6,))],
        compiler_params=pltpu.CompilerParams(vmem_limit_bytes=1 << 20),
    )(*(pltpu.with_memory_space_constraint(x, pltpu.VMEM) for x in held))
    half_up = half_up.reshape(n * rows, L)
    next_up = new_up.reshape(rows, L)
    next_down = new_down.reshape(rows, L).T
    return (half_up, half_down, half_norm, half_bias, next_up, next_down, next_norm, next_bias)


def solution(mesh):
    return jax.shard_map(
        on_device,
        mesh=mesh,
        in_specs=(
            P(("ens", "batch"), None, "cols"),
            P(("ens", "batch"), "cols", None),
            P(("ens", "batch"), None),
            P(("ens", "batch"), None),
            P(("ens", "batch"), "cols"),
            P(("ens", "cols"), "batch"),
            P(("ens", "batch")),
            P(("ens", "batch")),
        ),
        out_specs=(
            P("ens", "cols"),
            P(("ens", "cols"), None),
            P("ens"),
            P("ens"),
            P(("ens", "batch"), "cols"),
            P(("ens", "cols"), "batch"),
            P(("ens", "batch")),
            P(("ens", "batch")),
        ),
        check_vma=False,
    )
```

```python
import functools
import math

import jax
import jax.numpy as jnp
from jax import lax
from jax.experimental import pallas as pl
from jax.experimental.pallas import tpu as pltpu
from jax.sharding import PartitionSpec as P

learn_rate = 0.4
MESH = pl.DeviceIdType.MESH
R = 8
LANE = 128
SPLIT = 0.6
HEAD, TAIL = 1, 1
DEPTH = 4
SENDS = 2
LAST, LAST_SPLIT = 8, 0.7
FIRST, FIRST_SPLIT = 4, 0.7
VMEM_BYTES = 66_000_000
F32, BF16 = jnp.float32, jnp.bfloat16


def kernel(
    n,
    m,
    LA,
    LW,
    LF,
    up_ref,
    down_ref,
    pup_ref,
    pdown_ref,
    norm_ref,
    bias_ref,
    pnorm_ref,
    pbias_ref,
    G,
    T,
    NX,
    half_norm_ref,
    half_bias_ref,
    next_norm_ref,
    next_bias_ref,
    stage,
    turn,
    XA,
    XB,
    RYA,
    RYB,
    RZA,
    RZB,
    XA1,
    XB1,
    RYA1,
    RYB1,
    RZA1,
    RZB1,
    PR,
    SQ,
    V,
    VP,
    VY,
    VZ,
    up_sem,
    down_sem,
    par_sem,
    send,
    recv,
    first_recv,
    sum_recv,
    gather_recv,
    gather_send,
    sq_send,
    sq_recv,
    v_send,
    v_recv,
):
    Z = n // 2
    C = NX.shape[0]
    CH = C // 2
    H0 = CH // 2
    L = NX.shape[2]
    me = lax.axis_index("batch")
    core = lax.axis_index("cols")
    z = me // 2
    y = me % 2
    other = z * 2 + 1 - y
    rate = n ** (-0.5)

    def slot(p):
        return jnp.where(p < H0, p, jnp.where(p < H0 + CH, p - H0 + CH, p - CH))

    def load_up(c):
        return pltpu.make_async_copy(up_ref.at[:, :, c], stage.at[c % 2], up_sem.at[c % 2])

    blocks = L // LANE
    share = -(-blocks // H0)
    back = -(-blocks // (CH - H0))

    def load_down(b):
        return pltpu.make_async_copy(
            down_ref.at[pl.ds(b * LANE, LANE)], turn.at[b % DEPTH], down_sem.at[b % DEPTH]
        )

    def turn_block(b):
        def pieces(store):
            for j in range(n * CH * R // LANE):
                tile = turn[b % DEPTH, :, j * LANE : (j + 1) * LANE].T
                for i in range(LANE // R):
                    piece = j * (LANE // R) + i
                    d, k = piece // CH, piece % CH
                    store(d // 2, d % 2, CH + k, tile[i * R : (i + 1) * R].astype(BF16))

        @pl.when(b * LANE < LA)
        def _():
            at = pl.ds(pl.multiple_of(b * LANE, LANE), LANE)

            def store(d, v, c, x):
                XA[c, v, d, :, at] = x

            pieces(store)

        @pl.when(b * LANE >= LA)
        def _():
            at = pl.ds(pl.multiple_of(b * LANE - LA, LANE), LANE)

            def store(d, v, c, x):
                XB[c, d, v, :, at] = x

            pieces(store)

    def load_params():
        return [
            pltpu.make_async_copy(pup_ref, PR.at[pl.ds(0, CH)], par_sem.at[0]),
            pltpu.make_async_copy(pdown_ref, PR.at[pl.ds(CH, CH)], par_sem.at[1]),
        ]

    def load_vectors():
        return [
            pltpu.make_async_copy(norm_ref, V.at[0], par_sem.at[2]),
            pltpu.make_async_copy(bias_ref, V.at[1], par_sem.at[3]),
            pltpu.make_async_copy(pnorm_ref, VP.at[0], par_sem.at[4]),
            pltpu.make_async_copy(pbias_ref, VP.at[1], par_sem.at[5]),
        ]

    load_up(0).start()
    for d in load_params() + load_vectors():
        d.start()

    for b in range(min(DEPTH - 1, blocks)):
        load_down(b).start()

    barrier = pltpu.get_barrier_semaphore()
    def greet(to):
        pl.semaphore_signal(barrier, inc=1, device_id={"batch": to}, device_id_type=MESH)

    greet(other)

    @pl.when(z > 0)
    def _():
        greet(me - 2)

    @pl.when(z < Z - 1)
    def _():
        greet(me + 2)

    for o in range(1, m):
        pl.semaphore_signal(
            barrier, inc=1, device_id={"cols": (core + o) % m}, device_id_type=MESH
        )
    pl.semaphore_wait(barrier, jnp.where((z == 0) | (z == Z - 1), m + 1, m + 2))

    waits = recv.shape[1]

    def remote(src, dst, kind, p, to):
        return pltpu.make_async_remote_copy(
            src_ref=src,
            dst_ref=dst,
            send_sem=send.at[kind, p % SENDS],
            recv_sem=recv.at[kind, p % waits],
            device_id={"batch": to},
            device_id_type=MESH,
        )

    def free(copy, p):
        @pl.when(p >= SENDS)
        def _():
            copy(p - SENDS).wait_send()

    def go(copy, p):
        free(copy, p)
        copy(p).start()

    rest = (LA, XA, XB, RYA, RYB, RZA, RZB)
    start = (LF, XA1, XB1, RYA1, RYB1, RZA1, RZB1)

    def bufs(p, act):
        @pl.when(p >= FIRST)
        def _():
            act(rest)

        @pl.when(p < FIRST)
        def _():
            act(start)

    def free_sum(copy, p):
        @pl.when(p >= SENDS)
        def _():
            bufs(p - SENDS, lambda w: copy(p - SENDS, w).wait_send())

    def go_sum(copy, p):
        free_sum(copy, p)
        bufs(p, lambda w: copy(p, w).start())

    def wide(p):
        return p >= C - LAST

    def split(p, act):
        @pl.when(jnp.logical_not(wide(p)))
        def _():
            act(LA)

        @pl.when(wide(p))
        def _():
            act(LW)

    def free_split(copy, p):
        @pl.when(p >= SENDS)
        def _():
            split(p - SENDS, lambda la: copy(p - SENDS, la).wait_send())

    def go_split(copy, p):
        free_split(copy, p)
        split(p, lambda la: copy(p, la).start())

    def vec_y():
        return pltpu.make_async_remote_copy(
            src_ref=VZ.at[z],
            dst_ref=VY,
            send_sem=v_send.at[0],
            recv_sem=v_recv.at[0],
            device_id={"batch": other},
            device_id_type=MESH,
        )

    def vec_z(side, lo, count, to):
        ref = VZ.at[pl.ds(lo, count)]
        return pltpu.make_async_remote_copy(
            src_ref=ref,
            dst_ref=ref,
            send_sem=v_send.at[side],
            recv_sem=v_recv.at[side],
            device_id={"batch": to},
            device_id_type=MESH,
        )

    def vec_right(k):
        return vec_z(1, 0, k + 1, jnp.minimum(me + 2, n - 1))

    def vec_left(k):
        return vec_z(2, k, Z - k, jnp.maximum(me - 2, 0))

    def vec_step(t):
        for k in range(Z):

            @pl.when((z == k) & (t == k))
            def _():
                if k > 0:
                    vec_right(k - 1).wait_recv()
                if k < Z - 1:
                    vec_right(k).start()

            @pl.when((z == k) & (t == Z - 1 - k))
            def _():
                if k < Z - 1:
                    vec_left(k + 1).wait_recv()
                if k > 0:
                    vec_left(k).start()

            @pl.when((z == k) & (t == Z))
            def _():
                if k < Z - 1:
                    vec_right(k).wait_send()
                if k > 0:
                    vec_left(k).wait_send()

        @pl.when(t == Z)
        def _():
            total = VZ[0]
            for k in range(1, Z):
                total = total + VZ[k]
            width = VZ.shape[2]
            rows = width // n
            whole = total[2:4] - learn_rate * (total[0:2] * rate)
            halves = whole.astype(BF16)
            half_norm_ref[...] = halves[0:1].reshape(width)
            half_bias_ref[...] = halves[1:2].reshape(width)
            own = pltpu.roll(whole, (n - me) % n * rows, 1)[:, :rows]
            next_norm_ref[...] = own[0:1].reshape(rows)
            next_bias_ref[...] = own[1:2].reshape(rows)

    def sq_copy(p, o):
        return pltpu.make_async_remote_copy(
            src_ref=SQ.at[slot(p), 0],
            dst_ref=SQ.at[slot(p), o],
            send_sem=sq_send.at[o - 1, p % SENDS],
            recv_sem=sq_recv.at[o - 1, p % waits],
            device_id={"cols": (core + o) % m},
            device_id_type=MESH,
        )

    YA, YB, RA, LFA, RB, LFB, GYA, GYB, GRA, GLA, GRB, GLB = range(12)

    def ya(p, w):
        c = slot(p)
        return remote(w[1].at[c, 1 - y], w[3].at[c], YA, p, other)

    def yb(p, w):
        c = slot(p)
        return remote(w[2].at[c, z, 1 - y], w[4].at[c], YB, p, other)

    def gya(p, la):
        ref = G.at[:, y, slot(p), :, pl.ds(0, la)]
        return remote(ref, ref, GYA, p, other)

    def gya_in(p, la):
        ref = G.at[:, 1 - y, slot(p), :, pl.ds(0, la)]
        return remote(ref, ref, GYA, p, other)

    def gyb(p, la):
        ref = G.at[z, y, slot(p), :, pl.ds(la, L - la)]
        return remote(ref, ref, GYB, p, other)

    def gyb_in(p, la):
        ref = G.at[z, 1 - y, slot(p), :, pl.ds(la, L - la)]
        return remote(ref, ref, GYB, p, other)

    def head(p):
        return p < HEAD

    def tail(p):
        return p >= C - TAIL

    def right_of():
        return jnp.minimum(me + 2, n - 1)

    def left_of():
        return jnp.maximum(me - 2, 0)

    def piece(src, dst, send_sem, recv_sem, to):
        return pltpu.make_async_remote_copy(
            src_ref=src,
            dst_ref=dst,
            send_sem=send_sem,
            recv_sem=recv_sem,
            device_id={"batch": to},
            device_id_type=MESH,
        )

    def ya_piece(p, d):
        c = slot(p)
        return piece(
            XA1.at[c, 1 - y, d],
            RYA1.at[c, d],
            send.at[YA, p % SENDS],
            first_recv.at[p, d],
            other,
        )

    def take(p, d):
        c = slot(p)
        ya_piece(p, d).wait_recv()
        XA1[c, y, d] = (XA1[c, y, d].astype(F32) + RYA1[c, d].astype(F32)).astype(BF16)

    inward = [d for i in range(Z // 2) for d in (Z - 1 - i, i)]

    def sum_piece(first, right, p, d):
        c = slot(p)
        rz = RZA1 if first else RZB1
        kind = (RA if first else RB) if right else (LFA if first else LFB)
        return piece(
            XA1.at[c, y, d] if first else XB1.at[c, d],
            rz.at[c, d + 1 if right else d],
            send.at[kind, p % SENDS],
            sum_recv.at[2 * first + right, p, d],
            right_of() if right else left_of(),
        )

    def gather_piece(first, right, p, d):
        kind = (GRA if first else GRB) if right else (GLA if first else GLB)
        if first:
            ref = G.at[d, y, slot(p), :, pl.ds(0, LW)]
        else:
            ref = G.at[d, :, slot(p), :, pl.ds(LW, L - LW)]
        return piece(
            ref,
            ref,
            send.at[kind, p % SENDS],
            gather_recv.at[2 * first + right, p - (C - TAIL), d],
            right_of() if right else left_of(),
        )

    def gya_piece(p, d, v):
        ref = G.at[d, v, slot(p), :, pl.ds(0, LW)]
        e = p - (C - TAIL)
        return piece(ref, ref, gather_send.at[e, d], gather_recv.at[4, e, d], other)

    def x_ref(first, c, w):
        return w[1].at[c, y] if first else w[2].at[c]

    def sum_right(first, p, k, w):
        c = slot(p)
        return remote(
            x_ref(first, c, w).at[pl.ds(k + 1, Z - 1 - k)],
            w[5 if first else 6].at[c, pl.ds(k + 2, Z - 1 - k)],
            RA if first else RB,
            p,
            right_of(),
        )

    def sum_left(first, p, k, w):
        c = slot(p)
        return remote(
            x_ref(first, c, w).at[pl.ds(0, k)],
            w[5 if first else 6].at[c, pl.ds(0, k)],
            LFA if first else LFB,
            p,
            left_of(),
        )

    def add(first, p, lo, count, at, w):
        c = slot(p)
        x, rz = (w[1], w[5]) if first else (w[2], w[6])
        for d in range(count):
            i = (c, y, lo + d) if first else (c, lo + d)
            x[i] = (x[i].astype(F32) + rz[c, at + d].astype(F32)).astype(BF16)

    def at_hop(t, k, bulk, pieces, special):
        for right in (True, False):
            p = t - k if right else t - (Z - 1 - k)
            here = (z == k) & (p >= 0) & (p < C)

            @pl.when(here & jnp.logical_not(special(p)))
            def _():
                bulk(right, p)

            @pl.when(here & special(p))
            def _():
                pieces(right, p)

    def reduce_step(first, t):
        for k in range(Z):

            def to_right(p, w):
                return sum_right(first, p, k, w)

            def to_left(p, w):
                return sum_left(first, p, k, w)

            def bulk(right, p):
                def arrive(w):
                    if right:
                        sum_right(first, p, k - 1, w).wait_recv()
                        add(first, p, k, Z - k, k + 1, w)
                    else:
                        sum_left(first, p, k + 1, w).wait_recv()
                        add(first, p, 0, k + 1, 0, w)

                if k > 0 if right else k < Z - 1:
                    bufs(p, arrive)
                if k < Z - 1 if right else k > 0:
                    go_sum(to_right if right else to_left, p)

            def pieces(right, p):
                if k < Z - 1 if right else k > 0:
                    free_sum(to_right if right else to_left, p)
                for d in range(Z - 1, k - 1, -1) if right else range(k + 1):
                    if first and k == (0 if right else Z - 1):
                        take(p, d)
                    if k > 0 if right else k < Z - 1:
                        sum_piece(first, right, p, d).wait_recv()
                        add(first, p, d, 1, d + 1 if right else d, start)
                    if d != k:
                        sum_piece(first, right, p, d).start()

            at_hop(t, k, bulk, pieces, head)

    def g_ref(first, c, lo, count, la):
        at = pl.ds(lo, count)
        if first:
            return G.at[at, y, c, :, pl.ds(0, la)]
        return G.at[at, :, c, :, pl.ds(la, L - la)]

    def gather_right(first, p, k, la):
        ref = g_ref(first, slot(p), 0, k + 1, la)
        return remote(ref, ref, GRA if first else GRB, p, right_of())

    def gather_left(first, p, k, la):
        ref = g_ref(first, slot(p), k, Z - k, la)
        return remote(ref, ref, GLA if first else GLB, p, left_of())

    def gather_step(first, t):
        for k in range(Z):

            def to_right(p, la):
                return gather_right(first, p, k, la)

            def to_left(p, la):
                return gather_left(first, p, k, la)

            def bulk(right, p):
                if right:
                    if k > 0:
                        split(p, lambda la: gather_right(first, p, k - 1, la).wait_recv())
                    if k < Z - 1:
                        go_split(to_right, p)
                else:
                    if k < Z - 1:
                        split(p, lambda la: gather_left(first, p, k + 1, la).wait_recv())
                    if k > 0:
                        go_split(to_left, p)

            def pieces(right, p):
                on = k < Z - 1 if right else k > 0
                if on:
                    free_split(to_right if right else to_left, p)
                for d in range(k, -1, -1) if right else range(k, Z):
                    if d != k:
                        gather_piece(first, right, p, d).wait_recv()
                    if on:
                        gather_piece(first, right, p, d).start()
                    if first and d != k:
                        gya_piece(p, d, y).start()

            at_hop(t, k, bulk, pieces, tail)

    def last_sends(p):
        for copy in (ya(p, rest), yb(p, rest), gyb(p, LW)):
            copy.wait_send()
        for o in range(1, m):
            sq_copy(p, o).wait_send()
        for k in range(Z):

            @pl.when(z == k)
            def _():
                for first in (True, False):
                    if k < Z - 1:
                        sum_right(first, p, k, rest).wait_send()
                        gather_right(first, p, k, LW).wait_send()
                    if k > 0:
                        sum_left(first, p, k, rest).wait_send()
                        gather_left(first, p, k, LW).wait_send()

    def back_block(b):
        at = pl.ds(pl.multiple_of(b * LANE, LANE), LANE)
        for j in range(n * CH * R // LANE):
            rows = []
            for i in range(LANE // R):
                piece = j * (LANE // R) + i
                d, k = piece // CH, piece % CH
                rows.append(G[d // 2, d % 2, CH + k, :, at].astype(F32))
            tile = jnp.concatenate(rows, axis=0)
            T[at, j * LANE : (j + 1) * LANE] = tile.T.astype(BF16)

    def lanes(x):
        s = x[:, :LANE] * x[:, :LANE]
        for i in range(1, L // LANE):
            part = x[:, i * LANE : (i + 1) * LANE]
            s = s + part * part
        return s

    def when_chunk(c):
        return pl.when((c >= 0) & (c < C))

    def next_block(b):
        @pl.when(b + DEPTH - 1 < blocks)
        def _():
            load_down(b + DEPTH - 1).start()

        load_down(b).wait()
        turn_block(b)

    @pl.loop(0, C + 2 * Z)
    def _(t):
        def load_at(p, act):
            @pl.when((p < H0) | ((p >= H0 + CH) & (p < C)))
            def _():
                act(slot(p))

        load_at(t + 1, lambda c: load_up(c).start())

        def cast(c):
            load_up(c).wait()

            def put(w):
                for d in range(Z):
                    for v in range(2):
                        w[1][c, v, d] = stage[c % 2, d, v, :, : w[0]].astype(BF16)
                        w[2][c, d, v] = stage[c % 2, d, v, :, w[0] :].astype(BF16)

            bufs(t, put)

        load_at(t, cast)

        @pl.when((t < C) & jnp.logical_not(head(t)))
        def _():
            go_sum(ya, t)

        @pl.when(head(t))
        def _():
            free_sum(ya, t)
            for half in range(2):

                @pl.when(z // (Z // 2) == half)
                def _():
                    for d in inward:
                        ya_piece(t, Z - 1 - d if half else d).start()

        reduce_step(False, t)
        s = t - 1

        @pl.when((s >= 0) & head(s) & (z > 0) & (z < Z - 1))
        def _():
            for d in range(Z):
                take(s, d)

        @pl.when((s < C) & jnp.logical_not(head(s)))
        def _():
            c = slot(s)

            def arrive(w):
                ya(s, w).wait_recv()
                for d in range(Z):
                    w[1][c, y, d] = (
                        w[1][c, y, d].astype(F32) + w[3][c, d].astype(F32)
                    ).astype(BF16)

            bufs(s, arrive)

        reduce_step(True, s)
        b = t - (Z - 1)

        @when_chunk(b)
        def _():
            go_sum(yb, b)

        u = t - Z

        @pl.when(u == 0)
        def _():
            for d in load_params():
                d.wait()

        @when_chunk(u)
        def _():
            f = slot(u)

            def arrive(w):
                la = w[0]
                yb(u, w).wait_recv()
                NX[f, :, :la] = w[1][f, y, z].astype(F32) * rate
                NX[f, :, la:] = (w[2][f, z, y].astype(F32) + w[4][f].astype(F32)) * rate

            bufs(u, arrive)
            SQ[f, 0, 0] = lanes(NX[f])
            SQ[f, 0, 1] = lanes(PR[f])
            for o in range(1, m):
                go(lambda p, o=o: sq_copy(p, o), u)

        @when_chunk(u - 1)
        def _():
            split(u - 1, lambda la: gyb_in(u - 1, la).wait_recv())

        gather_step(False, u - 1)
        e = u - Z

        @when_chunk(u)
        def _():
            f = slot(u)
            for o in range(1, m):
                sq_copy(u, o).wait_recv()
            g = SQ[f, 0, 0]
            p = SQ[f, 0, 1]
            for o in range(1, m):
                g = g + SQ[f, o, 0]
                p = p + SQ[f, o, 1]
            g = jnp.sum(g, axis=1, keepdims=True)
            p = jnp.sum(p, axis=1, keepdims=True)
            scale = learn_rate * (jnp.sqrt(p) * lax.rsqrt(g + 1e-06))
            new = PR[f] - NX[f] * scale
            NX[f] = new
            G[z, y, f] = new.astype(BF16)
            go_split(gyb, u)

            @pl.when(tail(u))
            def _():
                gya_piece(u, z, y).start()

        gather_step(True, u)

        w = u - (Z - 1)

        @pl.when((w >= 0) & jnp.logical_not(tail(w)))
        def _():
            go_split(gya, w)

        @pl.when(t == 0)
        def _():
            for d in load_vectors():
                d.wait()
            width = VY.shape[1]
            place = jnp.zeros((1, width - VP.shape[2]), F32)
            for i in range(2):
                VZ[z, i : i + 1] = V[i]
                own = jnp.concatenate([VP[i], place], axis=1)
                VZ[z, 2 + i : 3 + i] = pltpu.roll(own, me * VP.shape[2], 1)
            vec_y().start()

        @pl.when(t == 2)
        def _():
            vec_y().wait()
            VZ[z] = VZ[z] + VY[...]

        vec_step(t - 3)

        @pl.when((e >= 0) & jnp.logical_not(tail(e)))
        def _():
            split(e, lambda la: gya_in(e, la).wait_recv())

        @pl.when((e < C) & tail(e))
        def _():
            for d in range(Z):
                gya_piece(e, d, 1 - y).wait_recv()
                gya_piece(e, d, y).wait_send()

        for i in range(share):
            b = t * share + i

            @pl.when(b < blocks)
            def _():
                next_block(b)

        for i in range(back):
            w = (t - (H0 + CH + 2 * Z)) * back + i

            @pl.when((w >= 0) & (w < blocks))
            def _():
                back_block(w)

    for i in range(SENDS):
        last_sends(C - SENDS + i)
        gya(C - TAIL - SENDS + i, LW).wait_send()


def put_kernel(
    G,
    T,
    NX,
    half_norm,
    half_bias,
    next_norm,
    next_bias,
    half_up_ref,
    half_down_ref,
    half_norm_ref,
    half_bias_ref,
    next_up_ref,
    next_down_ref,
    next_norm_ref,
    next_bias_ref,
    sem,
):
    Z = G.shape[0]
    CH = G.shape[2] // 2
    part = T.shape[0] // (2 * Z)
    copies = []

    def put(src, dst):
        d = pltpu.make_async_copy(src, dst, sem.at[len(copies)])
        d.start()
        copies.append(d)

    for k in range(Z):
        for v in range(2):
            put(G.at[k, v, pl.ds(0, CH)], half_up_ref.at[k, v])
            at = pl.ds((2 * k + v) * part, part)
            put(T.at[at], half_down_ref.at[at])
    put(NX.at[pl.ds(0, CH)], next_up_ref)
    put(NX.at[pl.ds(CH, CH)], next_down_ref)
    put(half_norm, half_norm_ref)
    put(half_bias, half_bias_ref)
    put(next_norm, next_norm_ref)
    put(next_bias, next_bias_ref)
    for d in copies:
        d.wait()


def on_device(
    slope_up, slope_down, slope_norm, slope_bias, param_up, param_down, param_norm, param_bias
):
    n = lax.axis_size("batch")
    m = lax.axis_size("cols")
    Z = n // 2
    rows, L = param_up.shape
    CH = rows // R
    C = 2 * CH
    LA = max(1, round(SPLIT * L / LANE)) * LANE
    LB = L - LA
    LF = min(L // LANE - 1, round(FIRST_SPLIT * L / LANE)) * LANE
    LW = min(L // LANE - 1, round(LAST_SPLIT * L / LANE)) * LANE
    width = slope_norm.shape[1]
    up = slope_up[0].reshape(Z, 2, CH, R, L)
    down = slope_down[0]
    pup = param_up.reshape(CH, R, L)
    pdown = param_down.T.reshape(CH, R, L)
    pnorm = param_norm.reshape(1, rows)
    pbias = param_bias.reshape(1, rows)
    hbm = pl.BlockSpec(memory_space=pl.ANY)
    vmem = pl.BlockSpec(memory_space=pltpu.VMEM)
    kept = [((Z, 2, C, R, L), BF16), ((L, n * rows), BF16), ((C, R, L), F32)]
    kept += [((width,), BF16)] * 2 + [((rows,), F32)] * 2
    size = sum(jnp.dtype(dtype).itemsize * math.prod(shape) for shape, dtype in kept)
    held = pl.pallas_call(
        functools.partial(kernel, n, m, LA, LW, LF),
        out_shape=tuple(pltpu.VMEM(shape, dtype) for shape, dtype in kept),
        in_specs=[hbm] * 8,
        out_specs=(vmem,) * 7,
        scratch_shapes=[
            pltpu.VMEM((2, Z, 2, R, L), F32),
            pltpu.VMEM((DEPTH, LANE, n * rows), F32),
            pltpu.VMEM((C, 2, Z, R, LA), BF16),
            pltpu.VMEM((C, Z, 2, R, LB), BF16),
            pltpu.VMEM((C, Z, R, LA), BF16),
            pltpu.VMEM((C, R, LB), BF16),
            pltpu.VMEM((C, Z + 1, R, LA), BF16),
            pltpu.VMEM((C, Z + 1, 2, R, LB), BF16),
            pltpu.VMEM((FIRST, 2, Z, R, LF), BF16),
            pltpu.VMEM((FIRST, Z, 2, R, L - LF), BF16),
            pltpu.VMEM((FIRST, Z, R, LF), BF16),
            pltpu.VMEM((FIRST, R, L - LF), BF16),
            pltpu.VMEM((FIRST, Z + 1, R, LF), BF16),
            pltpu.VMEM((FIRST, Z + 1, 2, R, L - LF), BF16),
            pltpu.VMEM((C, R, L), F32),
            pltpu.VMEM((C, m, 2, R, LANE), F32),
            pltpu.VMEM((2, 1, width), F32),
            pltpu.VMEM((2, 1, rows), F32),
            pltpu.VMEM((4, width), F32),
            pltpu.VMEM((Z, 4, width), F32),
            pltpu.SemaphoreType.DMA((2,)),
            pltpu.SemaphoreType.DMA((DEPTH,)),
            pltpu.SemaphoreType.DMA((6,)),
            pltpu.SemaphoreType.DMA((12, SENDS)),
            pltpu.SemaphoreType.DMA((12, Z + 1)),
            pltpu.SemaphoreType.DMA((HEAD, Z)),
            pltpu.SemaphoreType.DMA((4, HEAD, Z)),
            pltpu.SemaphoreType.DMA((5, TAIL, Z)),
            pltpu.SemaphoreType.DMA((TAIL, Z)),
            pltpu.SemaphoreType.DMA((m - 1, SENDS)),
            pltpu.SemaphoreType.DMA((m - 1, Z + 1)),
            pltpu.SemaphoreType.DMA((3,)),
            pltpu.SemaphoreType.DMA((3,)),
        ],
        compiler_params=pltpu.CompilerParams(
            collective_id=0, has_side_effects=True, vmem_limit_bytes=VMEM_BYTES - size
        ),
    )(up, down, pup, pdown, slope_norm, slope_bias, pnorm, pbias)
    half_up, half_down, half_norm, half_bias, new_up, new_down, next_norm, next_bias = pl.pallas_call(
        put_kernel,
        out_shape=(
            jax.ShapeDtypeStruct((Z, 2, CH, R, L), BF16),
            jax.ShapeDtypeStruct((L, n * rows), BF16),
            jax.ShapeDtypeStruct((width,), BF16),
            jax.ShapeDtypeStruct((width,), BF16),
            jax.ShapeDtypeStruct((CH, R, L), F32),
            jax.ShapeDtypeStruct((CH, R, L), F32),
            jax.ShapeDtypeStruct((rows,), F32),
            jax.ShapeDtypeStruct((rows,), F32),
        ),
        in_specs=[vmem] * 7,
        out_specs=(hbm,) * 8,
        scratch_shapes=[pltpu.SemaphoreType.DMA((4 * Z + 6,))],
        compiler_params=pltpu.CompilerParams(vmem_limit_bytes=1 << 20),
    )(*(pltpu.with_memory_space_constraint(x, pltpu.VMEM) for x in held))
    half_up = half_up.reshape(n * rows, L)
    next_up = new_up.reshape(rows, L)
    next_down = new_down.reshape(rows, L).T
    return (half_up, half_down, half_norm, half_bias, next_up, next_down, next_norm, next_bias)


def solution(mesh):
    return jax.shard_map(
        on_device,
        mesh=mesh,
        in_specs=(
            P(("ens", "batch"), None, "cols"),
            P(("ens", "batch"), "cols", None),
            P(("ens", "batch"), None),
            P(("ens", "batch"), None),
            P(("ens", "batch"), "cols"),
            P(("ens", "cols"), "batch"),
            P(("ens", "batch")),
            P(("ens", "batch")),
        ),
        out_specs=(
            P("ens", "cols"),
            P(("ens", "cols"), None),
            P("ens"),
            P("ens"),
            P(("ens", "batch"), "cols"),
            P(("ens", "cols"), "batch"),
            P(("ens", "batch")),
            P(("ens", "batch")),
        ),
        check_vma=False,
    )
```

```python
import functools
import math

import jax
import jax.numpy as jnp
from jax import lax
from jax.experimental import pallas as pl
from jax.experimental.pallas import tpu as pltpu
from jax.sharding import PartitionSpec as P

learn_rate = 0.4
MESH = pl.DeviceIdType.MESH
R = 8
LANE = 128
SPLIT = 0.6
HEAD, TAIL = 1, 1
DEPTH = 4
SENDS = 2
LAST, LAST_SPLIT = 8, 0.7
FIRST, FIRST_SPLIT = 4, 0.7
VMEM_BYTES = 66_000_000
F32, BF16 = jnp.float32, jnp.bfloat16


def kernel(
    n,
    m,
    LA,
    LW,
    LF,
    up_ref,
    down_ref,
    pup_ref,
    pdown_ref,
    norm_ref,
    bias_ref,
    pnorm_ref,
    pbias_ref,
    G,
    T,
    NX,
    half_norm_ref,
    half_bias_ref,
    next_norm_ref,
    next_bias_ref,
    stage,
    turn,
    XA,
    XB,
    RYA,
    RYB,
    RZA,
    RZB,
    XA1,
    XB1,
    RYA1,
    RYB1,
    RZA1,
    RZB1,
    PR,
    SQ,
    V,
    VP,
    VY,
    VZ,
    up_sem,
    down_sem,
    par_sem,
    send,
    recv,
    first_recv,
    sum_recv,
    gather_recv,
    gather_send,
    sq_send,
    sq_recv,
    v_send,
    v_recv,
):
    Z = n // 2
    C = NX.shape[0]
    CH = C // 2
    H0 = CH // 2
    L = NX.shape[2]
    me = lax.axis_index("batch")
    core = lax.axis_index("cols")
    z = me // 2
    y = me % 2
    other = z * 2 + 1 - y
    rate = n ** (-0.5)

    def slot(p):
        return jnp.where(p < H0, p, jnp.where(p < H0 + CH, p - H0 + CH, p - CH))

    def load_up(c):
        return pltpu.make_async_copy(up_ref.at[:, :, c], stage.at[c % 2], up_sem.at[c % 2])

    blocks = L // LANE
    share = -(-blocks // H0)
    back = -(-blocks // (CH - H0))

    def load_down(b):
        return pltpu.make_async_copy(
            down_ref.at[pl.ds(b * LANE, LANE)], turn.at[b % DEPTH], down_sem.at[b % DEPTH]
        )

    def turn_block(b):
        def pieces(store):
            for j in range(n * CH * R // LANE):
                tile = turn[b % DEPTH, :, j * LANE : (j + 1) * LANE].T
                for i in range(LANE // R):
                    piece = j * (LANE // R) + i
                    d, k = piece // CH, piece % CH
                    store(d // 2, d % 2, CH + k, tile[i * R : (i + 1) * R].astype(BF16))

        @pl.when(b * LANE < LA)
        def _():
            at = pl.ds(pl.multiple_of(b * LANE, LANE), LANE)

            def store(d, v, c, x):
                XA[c, v, d, :, at] = x

            pieces(store)

        @pl.when(b * LANE >= LA)
        def _():
            at = pl.ds(pl.multiple_of(b * LANE - LA, LANE), LANE)

            def store(d, v, c, x):
                XB[c, d, v, :, at] = x

            pieces(store)

    def load_params():
        return [
            pltpu.make_async_copy(pup_ref, PR.at[pl.ds(0, CH)], par_sem.at[0]),
            pltpu.make_async_copy(pdown_ref, PR.at[pl.ds(CH, CH)], par_sem.at[1]),
        ]

    def load_vectors():
        return [
            pltpu.make_async_copy(norm_ref, V.at[0], par_sem.at[2]),
            pltpu.make_async_copy(bias_ref, V.at[1], par_sem.at[3]),
            pltpu.make_async_copy(pnorm_ref, VP.at[0], par_sem.at[4]),
            pltpu.make_async_copy(pbias_ref, VP.at[1], par_sem.at[5]),
        ]

    load_up(0).start()

    barrier = pltpu.get_barrier_semaphore()
    def greet(to):
        pl.semaphore_signal(barrier, inc=1, device_id={"batch": to}, device_id_type=MESH)

    greet(other)

    @pl.when(z > 0)
    def _():
        greet(me - 2)

    @pl.when(z < Z - 1)
    def _():
        greet(me + 2)

    for o in range(1, m):
        pl.semaphore_signal(
            barrier, inc=1, device_id={"cols": (core + o) % m}, device_id_type=MESH
        )
    pl.semaphore_wait(barrier, jnp.where((z == 0) | (z == Z - 1), m + 1, m + 2))

    waits = recv.shape[1]

    def remote(src, dst, kind, p, to):
        return pltpu.make_async_remote_copy(
            src_ref=src,
            dst_ref=dst,
            send_sem=send.at[kind, p % SENDS],
            recv_sem=recv.at[kind, p % waits],
            device_id={"batch": to},
            device_id_type=MESH,
        )

    def free(copy, p):
        @pl.when(p >= SENDS)
        def _():
            copy(p - SENDS).wait_send()

    def go(copy, p):
        free(copy, p)
        copy(p).start()

    rest = (LA, XA, XB, RYA, RYB, RZA, RZB)
    start = (LF, XA1, XB1, RYA1, RYB1, RZA1, RZB1)

    def bufs(p, act):
        @pl.when(p >= FIRST)
        def _():
            act(rest)

        @pl.when(p < FIRST)
        def _():
            act(start)

    def free_sum(copy, p):
        @pl.when(p >= SENDS)
        def _():
            bufs(p - SENDS, lambda w: copy(p - SENDS, w).wait_send())

    def go_sum(copy, p):
        free_sum(copy, p)
        bufs(p, lambda w: copy(p, w).start())

    def wide(p):
        return p >= C - LAST

    def split(p, act):
        @pl.when(jnp.logical_not(wide(p)))
        def _():
            act(LA)

        @pl.when(wide(p))
        def _():
            act(LW)

    def free_split(copy, p):
        @pl.when(p >= SENDS)
        def _():
            split(p - SENDS, lambda la: copy(p - SENDS, la).wait_send())

    def go_split(copy, p):
        free_split(copy, p)
        split(p, lambda la: copy(p, la).start())

    def vec_y():
        return pltpu.make_async_remote_copy(
            src_ref=VZ.at[z],
            dst_ref=VY,
            send_sem=v_send.at[0],
            recv_sem=v_recv.at[0],
            device_id={"batch": other},
            device_id_type=MESH,
        )

    def vec_z(side, lo, count, to):
        ref = VZ.at[pl.ds(lo, count)]
        return pltpu.make_async_remote_copy(
            src_ref=ref,
            dst_ref=ref,
            send_sem=v_send.at[side],
            recv_sem=v_recv.at[side],
            device_id={"batch": to},
            device_id_type=MESH,
        )

    def vec_right(k):
        return vec_z(1, 0, k + 1, jnp.minimum(me + 2, n - 1))

    def vec_left(k):
        return vec_z(2, k, Z - k, jnp.maximum(me - 2, 0))

    def vec_step(t):
        for k in range(Z):

            @pl.when((z == k) & (t == k))
            def _():
                if k > 0:
                    vec_right(k - 1).wait_recv()
                if k < Z - 1:
                    vec_right(k).start()

            @pl.when((z == k) & (t == Z - 1 - k))
            def _():
                if k < Z - 1:
                    vec_left(k + 1).wait_recv()
                if k > 0:
                    vec_left(k).start()

            @pl.when((z == k) & (t == Z))
            def _():
                if k < Z - 1:
                    vec_right(k).wait_send()
                if k > 0:
                    vec_left(k).wait_send()

        @pl.when(t == Z)
        def _():
            total = VZ[0]
            for k in range(1, Z):
                total = total + VZ[k]
            width = VZ.shape[2]
            rows = width // n
            whole = total[2:4] - learn_rate * (total[0:2] * rate)
            halves = whole.astype(BF16)
            half_norm_ref[...] = halves[0:1].reshape(width)
            half_bias_ref[...] = halves[1:2].reshape(width)
            own = pltpu.roll(whole, (n - me) % n * rows, 1)[:, :rows]
            next_norm_ref[...] = own[0:1].reshape(rows)
            next_bias_ref[...] = own[1:2].reshape(rows)

    def sq_copy(p, o):
        return pltpu.make_async_remote_copy(
            src_ref=SQ.at[slot(p), 0],
            dst_ref=SQ.at[slot(p), o],
            send_sem=sq_send.at[o - 1, p % SENDS],
            recv_sem=sq_recv.at[o - 1, p % waits],
            device_id={"cols": (core + o) % m},
            device_id_type=MESH,
        )

    YA, YB, RA, LFA, RB, LFB, GYA, GYB, GRA, GLA, GRB, GLB = range(12)

    def ya(p, w):
        c = slot(p)
        return remote(w[1].at[c, 1 - y], w[3].at[c], YA, p, other)

    def yb(p, w):
        c = slot(p)
        return remote(w[2].at[c, z, 1 - y], w[4].at[c], YB, p, other)

    def gya(p, la):
        ref = G.at[:, y, slot(p), :, pl.ds(0, la)]
        return remote(ref, ref, GYA, p, other)

    def gya_in(p, la):
        ref = G.at[:, 1 - y, slot(p), :, pl.ds(0, la)]
        return remote(ref, ref, GYA, p, other)

    def gyb(p, la):
        ref = G.at[z, y, slot(p), :, pl.ds(la, L - la)]
        return remote(ref, ref, GYB, p, other)

    def gyb_in(p, la):
        ref = G.at[z, 1 - y, slot(p), :, pl.ds(la, L - la)]
        return remote(ref, ref, GYB, p, other)

    def head(p):
        return p < HEAD

    def tail(p):
        return p >= C - TAIL

    def right_of():
        return jnp.minimum(me + 2, n - 1)

    def left_of():
        return jnp.maximum(me - 2, 0)

    def piece(src, dst, send_sem, recv_sem, to):
        return pltpu.make_async_remote_copy(
            src_ref=src,
            dst_ref=dst,
            send_sem=send_sem,
            recv_sem=recv_sem,
            device_id={"batch": to},
            device_id_type=MESH,
        )

    def ya_piece(p, d):
        c = slot(p)
        return piece(
            XA1.at[c, 1 - y, d],
            RYA1.at[c, d],
            send.at[YA, p % SENDS],
            first_recv.at[p, d],
            other,
        )

    def take(p, d):
        c = slot(p)
        ya_piece(p, d).wait_recv()
        XA1[c, y, d] = (XA1[c, y, d].astype(F32) + RYA1[c, d].astype(F32)).astype(BF16)

    inward = [d for i in range(Z // 2) for d in (Z - 1 - i, i)]

    def sum_piece(first, right, p, d):
        c = slot(p)
        rz = RZA1 if first else RZB1
        kind = (RA if first else RB) if right else (LFA if first else LFB)
        return piece(
            XA1.at[c, y, d] if first else XB1.at[c, d],
            rz.at[c, d + 1 if right else d],
            send.at[kind, p % SENDS],
            sum_recv.at[2 * first + right, p, d],
            right_of() if right else left_of(),
        )

    def gather_piece(first, right, p, d):
        kind = (GRA if first else GRB) if right else (GLA if first else GLB)
        if first:
            ref = G.at[d, y, slot(p), :, pl.ds(0, LW)]
        else:
            ref = G.at[d, :, slot(p), :, pl.ds(LW, L - LW)]
        return piece(
            ref,
            ref,
            send.at[kind, p % SENDS],
            gather_recv.at[2 * first + right, p - (C - TAIL), d],
            right_of() if right else left_of(),
        )

    def gya_piece(p, d, v):
        ref = G.at[d, v, slot(p), :, pl.ds(0, LW)]
        e = p - (C - TAIL)
        return piece(ref, ref, gather_send.at[e, d], gather_recv.at[4, e, d], other)

    def x_ref(first, c, w):
        return w[1].at[c, y] if first else w[2].at[c]

    def sum_right(first, p, k, w):
        c = slot(p)
        return remote(
            x_ref(first, c, w).at[pl.ds(k + 1, Z - 1 - k)],
            w[5 if first else 6].at[c, pl.ds(k + 2, Z - 1 - k)],
            RA if first else RB,
            p,
            right_of(),
        )

    def sum_left(first, p, k, w):
        c = slot(p)
        return remote(
            x_ref(first, c, w).at[pl.ds(0, k)],
            w[5 if first else 6].at[c, pl.ds(0, k)],
            LFA if first else LFB,
            p,
            left_of(),
        )

    def add(first, p, lo, count, at, w):
        c = slot(p)
        x, rz = (w[1], w[5]) if first else (w[2], w[6])
        for d in range(count):
            i = (c, y, lo + d) if first else (c, lo + d)
            x[i] = (x[i].astype(F32) + rz[c, at + d].astype(F32)).astype(BF16)

    def at_hop(t, k, bulk, pieces, special):
        for right in (True, False):
            p = t - k if right else t - (Z - 1 - k)
            here = (z == k) & (p >= 0) & (p < C)

            @pl.when(here & jnp.logical_not(special(p)))
            def _():
                bulk(right, p)

            @pl.when(here & special(p))
            def _():
                pieces(right, p)

    def reduce_step(first, t):
        for k in range(Z):

            def to_right(p, w):
                return sum_right(first, p, k, w)

            def to_left(p, w):
                return sum_left(first, p, k, w)

            def bulk(right, p):
                def arrive(w):
                    if right:
                        sum_right(first, p, k - 1, w).wait_recv()
                        add(first, p, k, Z - k, k + 1, w)
                    else:
                        sum_left(first, p, k + 1, w).wait_recv()
                        add(first, p, 0, k + 1, 0, w)

                if k > 0 if right else k < Z - 1:
                    bufs(p, arrive)
                if k < Z - 1 if right else k > 0:
                    go_sum(to_right if right else to_left, p)

            def pieces(right, p):
                if k < Z - 1 if right else k > 0:
                    free_sum(to_right if right else to_left, p)
                for d in range(Z - 1, k - 1, -1) if right else range(k + 1):
                    if first and k == (0 if right else Z - 1):
                        take(p, d)
                    if k > 0 if right else k < Z - 1:
                        sum_piece(first, right, p, d).wait_recv()
                        add(first, p, d, 1, d + 1 if right else d, start)
                    if d != k:
                        sum_piece(first, right, p, d).start()

            at_hop(t, k, bulk, pieces, head)

    def g_ref(first, c, lo, count, la):
        at = pl.ds(lo, count)
        if first:
            return G.at[at, y, c, :, pl.ds(0, la)]
        return G.at[at, :, c, :, pl.ds(la, L - la)]

    def gather_right(first, p, k, la):
        ref = g_ref(first, slot(p), 0, k + 1, la)
        return remote(ref, ref, GRA if first else GRB, p, right_of())

    def gather_left(first, p, k, la):
        ref = g_ref(first, slot(p), k, Z - k, la)
        return remote(ref, ref, GLA if first else GLB, p, left_of())

    def gather_step(first, t):
        for k in range(Z):

            def to_right(p, la):
                return gather_right(first, p, k, la)

            def to_left(p, la):
                return gather_left(first, p, k, la)

            def bulk(right, p):
                if right:
                    if k > 0:
                        split(p, lambda la: gather_right(first, p, k - 1, la).wait_recv())
                    if k < Z - 1:
                        go_split(to_right, p)
                else:
                    if k < Z - 1:
                        split(p, lambda la: gather_left(first, p, k + 1, la).wait_recv())
                    if k > 0:
                        go_split(to_left, p)

            def pieces(right, p):
                on = k < Z - 1 if right else k > 0
                if on:
                    free_split(to_right if right else to_left, p)
                for d in range(k, -1, -1) if right else range(k, Z):
                    if d != k:
                        gather_piece(first, right, p, d).wait_recv()
                    if on:
                        gather_piece(first, right, p, d).start()
                    if first and d != k:
                        gya_piece(p, d, y).start()

            at_hop(t, k, bulk, pieces, tail)

    def last_sends(p):
        for copy in (ya(p, rest), yb(p, rest), gyb(p, LW)):
            copy.wait_send()
        for o in range(1, m):
            sq_copy(p, o).wait_send()
        for k in range(Z):

            @pl.when(z == k)
            def _():
                for first in (True, False):
                    if k < Z - 1:
                        sum_right(first, p, k, rest).wait_send()
                        gather_right(first, p, k, LW).wait_send()
                    if k > 0:
                        sum_left(first, p, k, rest).wait_send()
                        gather_left(first, p, k, LW).wait_send()

    def back_block(b):
        at = pl.ds(pl.multiple_of(b * LANE, LANE), LANE)
        for j in range(n * CH * R // LANE):
            rows = []
            for i in range(LANE // R):
                piece = j * (LANE // R) + i
                d, k = piece // CH, piece % CH
                rows.append(G[d // 2, d % 2, CH + k, :, at].astype(F32))
            tile = jnp.concatenate(rows, axis=0)
            T[at, j * LANE : (j + 1) * LANE] = tile.T.astype(BF16)

    def lanes(x):
        s = x[:, :LANE] * x[:, :LANE]
        for i in range(1, L // LANE):
            part = x[:, i * LANE : (i + 1) * LANE]
            s = s + part * part
        return s

    def when_chunk(c):
        return pl.when((c >= 0) & (c < C))

    def next_block(b):
        @pl.when(b + DEPTH - 1 < blocks)
        def _():
            load_down(b + DEPTH - 1).start()

        load_down(b).wait()
        turn_block(b)

    @pl.loop(0, C + 2 * Z)
    def _(t):
        def load_at(p, act):
            @pl.when((p < H0) | ((p >= H0 + CH) & (p < C)))
            def _():
                act(slot(p))

        load_at(t + 1, lambda c: load_up(c).start())

        def cast(c):
            load_up(c).wait()

            def put(w):
                for d in range(Z):
                    for v in range(2):
                        w[1][c, v, d] = stage[c % 2, d, v, :, : w[0]].astype(BF16)
                        w[2][c, d, v] = stage[c % 2, d, v, :, w[0] :].astype(BF16)

            bufs(t, put)

        load_at(t, cast)

        @pl.when((t < C) & jnp.logical_not(head(t)))
        def _():
            go_sum(ya, t)

        @pl.when(head(t))
        def _():
            free_sum(ya, t)
            for half in range(2):

                @pl.when(z // (Z // 2) == half)
                def _():
                    for d in inward:
                        ya_piece(t, Z - 1 - d if half else d).start()

        reduce_step(False, t)
        s = t - 1

        @pl.when(t == 0)
        def _():
            for d in load_vectors():
                d.start()
            for b in range(min(DEPTH - 1, blocks)):
                load_down(b).start()
            for d in load_params():
                d.start()


        @pl.when((s >= 0) & head(s) & (z > 0) & (z < Z - 1))
        def _():
            for d in range(Z):
                take(s, d)

        @pl.when((s < C) & jnp.logical_not(head(s)))
        def _():
            c = slot(s)

            def arrive(w):
                ya(s, w).wait_recv()
                for d in range(Z):
                    w[1][c, y, d] = (
                        w[1][c, y, d].astype(F32) + w[3][c, d].astype(F32)
                    ).astype(BF16)

            bufs(s, arrive)

        reduce_step(True, s)
        b = t - (Z - 1)

        @when_chunk(b)
        def _():
            go_sum(yb, b)

        u = t - Z

        @pl.when(u == 0)
        def _():
            for d in load_params():
                d.wait()

        @when_chunk(u)
        def _():
            f = slot(u)

            def arrive(w):
                la = w[0]
                yb(u, w).wait_recv()
                NX[f, :, :la] = w[1][f, y, z].astype(F32) * rate
                NX[f, :, la:] = (w[2][f, z, y].astype(F32) + w[4][f].astype(F32)) * rate

            bufs(u, arrive)
            SQ[f, 0, 0] = lanes(NX[f])
            SQ[f, 0, 1] = lanes(PR[f])
            for o in range(1, m):
                go(lambda p, o=o: sq_copy(p, o), u)

        @when_chunk(u - 1)
        def _():
            split(u - 1, lambda la: gyb_in(u - 1, la).wait_recv())

        gather_step(False, u - 1)
        e = u - Z

        @when_chunk(u)
        def _():
            f = slot(u)
            for o in range(1, m):
                sq_copy(u, o).wait_recv()
            g = SQ[f, 0, 0]
            p = SQ[f, 0, 1]
            for o in range(1, m):
                g = g + SQ[f, o, 0]
                p = p + SQ[f, o, 1]
            g = jnp.sum(g, axis=1, keepdims=True)
            p = jnp.sum(p, axis=1, keepdims=True)
            scale = learn_rate * (jnp.sqrt(p) * lax.rsqrt(g + 1e-06))
            new = PR[f] - NX[f] * scale
            NX[f] = new
            G[z, y, f] = new.astype(BF16)
            go_split(gyb, u)

            @pl.when(tail(u))
            def _():
                gya_piece(u, z, y).start()

        gather_step(True, u)

        w = u - (Z - 1)

        @pl.when((w >= 0) & jnp.logical_not(tail(w)))
        def _():
            go_split(gya, w)

        @pl.when(t == 0)
        def _():
            for d in load_vectors():
                d.wait()
            width = VY.shape[1]
            place = jnp.zeros((1, width - VP.shape[2]), F32)
            for i in range(2):
                VZ[z, i : i + 1] = V[i]
                own = jnp.concatenate([VP[i], place], axis=1)
                VZ[z, 2 + i : 3 + i] = pltpu.roll(own, me * VP.shape[2], 1)
            vec_y().start()

        @pl.when(t == 2)
        def _():
            vec_y().wait()
            VZ[z] = VZ[z] + VY[...]

        vec_step(t - 3)

        @pl.when((e >= 0) & jnp.logical_not(tail(e)))
        def _():
            split(e, lambda la: gya_in(e, la).wait_recv())

        @pl.when((e < C) & tail(e))
        def _():
            for d in range(Z):
                gya_piece(e, d, 1 - y).wait_recv()
                gya_piece(e, d, y).wait_send()

        for i in range(share):
            b = t * share + i

            @pl.when(b < blocks)
            def _():
                next_block(b)

        for i in range(back):
            w = (t - (H0 + CH + 2 * Z)) * back + i

            @pl.when((w >= 0) & (w < blocks))
            def _():
                back_block(w)

    for i in range(SENDS):
        last_sends(C - SENDS + i)
        gya(C - TAIL - SENDS + i, LW).wait_send()


def put_kernel(
    G,
    T,
    NX,
    half_norm,
    half_bias,
    next_norm,
    next_bias,
    half_up_ref,
    half_down_ref,
    half_norm_ref,
    half_bias_ref,
    next_up_ref,
    next_down_ref,
    next_norm_ref,
    next_bias_ref,
    sem,
):
    Z = G.shape[0]
    CH = G.shape[2] // 2
    part = T.shape[0] // (2 * Z)
    copies = []

    def put(src, dst):
        d = pltpu.make_async_copy(src, dst, sem.at[len(copies)])
        d.start()
        copies.append(d)

    for k in range(Z):
        for v in range(2):
            put(G.at[k, v, pl.ds(0, CH)], half_up_ref.at[k, v])
            at = pl.ds((2 * k + v) * part, part)
            put(T.at[at], half_down_ref.at[at])
    put(NX.at[pl.ds(0, CH)], next_up_ref)
    put(NX.at[pl.ds(CH, CH)], next_down_ref)
    put(half_norm, half_norm_ref)
    put(half_bias, half_bias_ref)
    put(next_norm, next_norm_ref)
    put(next_bias, next_bias_ref)
    for d in copies:
        d.wait()


def on_device(
    slope_up, slope_down, slope_norm, slope_bias, param_up, param_down, param_norm, param_bias
):
    n = lax.axis_size("batch")
    m = lax.axis_size("cols")
    Z = n // 2
    rows, L = param_up.shape
    CH = rows // R
    C = 2 * CH
    LA = max(1, round(SPLIT * L / LANE)) * LANE
    LB = L - LA
    LF = min(L // LANE - 1, round(FIRST_SPLIT * L / LANE)) * LANE
    LW = min(L // LANE - 1, round(LAST_SPLIT * L / LANE)) * LANE
    width = slope_norm.shape[1]
    up = slope_up[0].reshape(Z, 2, CH, R, L)
    down = slope_down[0]
    pup = param_up.reshape(CH, R, L)
    pdown = param_down.T.reshape(CH, R, L)
    pnorm = param_norm.reshape(1, rows)
    pbias = param_bias.reshape(1, rows)
    hbm = pl.BlockSpec(memory_space=pl.ANY)
    vmem = pl.BlockSpec(memory_space=pltpu.VMEM)
    kept = [((Z, 2, C, R, L), BF16), ((L, n * rows), BF16), ((C, R, L), F32)]
    kept += [((width,), BF16)] * 2 + [((rows,), F32)] * 2
    size = sum(jnp.dtype(dtype).itemsize * math.prod(shape) for shape, dtype in kept)
    held = pl.pallas_call(
        functools.partial(kernel, n, m, LA, LW, LF),
        out_shape=tuple(pltpu.VMEM(shape, dtype) for shape, dtype in kept),
        in_specs=[hbm] * 8,
        out_specs=(vmem,) * 7,
        scratch_shapes=[
            pltpu.VMEM((2, Z, 2, R, L), F32),
            pltpu.VMEM((DEPTH, LANE, n * rows), F32),
            pltpu.VMEM((C, 2, Z, R, LA), BF16),
            pltpu.VMEM((C, Z, 2, R, LB), BF16),
            pltpu.VMEM((C, Z, R, LA), BF16),
            pltpu.VMEM((C, R, LB), BF16),
            pltpu.VMEM((C, Z + 1, R, LA), BF16),
            pltpu.VMEM((C, Z + 1, 2, R, LB), BF16),
            pltpu.VMEM((FIRST, 2, Z, R, LF), BF16),
            pltpu.VMEM((FIRST, Z, 2, R, L - LF), BF16),
            pltpu.VMEM((FIRST, Z, R, LF), BF16),
            pltpu.VMEM((FIRST, R, L - LF), BF16),
            pltpu.VMEM((FIRST, Z + 1, R, LF), BF16),
            pltpu.VMEM((FIRST, Z + 1, 2, R, L - LF), BF16),
            pltpu.VMEM((C, R, L), F32),
            pltpu.VMEM((C, m, 2, R, LANE), F32),
            pltpu.VMEM((2, 1, width), F32),
            pltpu.VMEM((2, 1, rows), F32),
            pltpu.VMEM((4, width), F32),
            pltpu.VMEM((Z, 4, width), F32),
            pltpu.SemaphoreType.DMA((2,)),
            pltpu.SemaphoreType.DMA((DEPTH,)),
            pltpu.SemaphoreType.DMA((6,)),
            pltpu.SemaphoreType.DMA((12, SENDS)),
            pltpu.SemaphoreType.DMA((12, Z + 1)),
            pltpu.SemaphoreType.DMA((HEAD, Z)),
            pltpu.SemaphoreType.DMA((4, HEAD, Z)),
            pltpu.SemaphoreType.DMA((5, TAIL, Z)),
            pltpu.SemaphoreType.DMA((TAIL, Z)),
            pltpu.SemaphoreType.DMA((m - 1, SENDS)),
            pltpu.SemaphoreType.DMA((m - 1, Z + 1)),
            pltpu.SemaphoreType.DMA((3,)),
            pltpu.SemaphoreType.DMA((3,)),
        ],
        compiler_params=pltpu.CompilerParams(
            collective_id=0, has_side_effects=True, vmem_limit_bytes=VMEM_BYTES - size
        ),
    )(up, down, pup, pdown, slope_norm, slope_bias, pnorm, pbias)
    half_up, half_down, half_norm, half_bias, new_up, new_down, next_norm, next_bias = pl.pallas_call(
        put_kernel,
        out_shape=(
            jax.ShapeDtypeStruct((Z, 2, CH, R, L), BF16),
            jax.ShapeDtypeStruct((L, n * rows), BF16),
            jax.ShapeDtypeStruct((width,), BF16),
            jax.ShapeDtypeStruct((width,), BF16),
            jax.ShapeDtypeStruct((CH, R, L), F32),
            jax.ShapeDtypeStruct((CH, R, L), F32),
            jax.ShapeDtypeStruct((rows,), F32),
            jax.ShapeDtypeStruct((rows,), F32),
        ),
        in_specs=[vmem] * 7,
        out_specs=(hbm,) * 8,
        scratch_shapes=[pltpu.SemaphoreType.DMA((4 * Z + 6,))],
        compiler_params=pltpu.CompilerParams(vmem_limit_bytes=1 << 20),
    )(*(pltpu.with_memory_space_constraint(x, pltpu.VMEM) for x in held))
    half_up = half_up.reshape(n * rows, L)
    next_up = new_up.reshape(rows, L)
    next_down = new_down.reshape(rows, L).T
    return (half_up, half_down, half_norm, half_bias, next_up, next_down, next_norm, next_bias)


def solution(mesh):
    return jax.shard_map(
        on_device,
        mesh=mesh,
        in_specs=(
            P(("ens", "batch"), None, "cols"),
            P(("ens", "batch"), "cols", None),
            P(("ens", "batch"), None),
            P(("ens", "batch"), None),
            P(("ens", "batch"), "cols"),
            P(("ens", "cols"), "batch"),
            P(("ens", "batch")),
            P(("ens", "batch")),
        ),
        out_specs=(
            P("ens", "cols"),
            P(("ens", "cols"), None),
            P("ens"),
            P("ens"),
            P(("ens", "batch"), "cols"),
            P(("ens", "cols"), "batch"),
            P(("ens", "batch")),
            P(("ens", "batch")),
        ),
        check_vma=False,
    )
```
